256 devices in a mesh: fiber: 128 (over z, y, x), wave: 2 (over core).
Axes of the slice: x: 4, y: 4, z: 8, core: 2. Of those that a mesh axis runs over, the one named last changes fastest.
Arguments:
- spectra: float32 [4, 5120, 8192], P(None, 'fiber', 'wave'), may hold values from 0 to 10
- inverse_var: float32 [4, 5120, 8192], P(None, 'fiber', 'wave'), may hold values from 0.1 to 10
- mask_bits: int32 [4, 5120, 8192], P(None, 'fiber', 'wave'), may hold values from 0 to 512, as said below
- sky_flags: int32 [4, 5120], P(None, 'fiber'), may hold values 0 or 1
- fiber_ids: int32 [5120], P('fiber'), may hold values from 0 to 5119, each once
- positions: float32 [2, 5120], replicated, may hold values from -1 to 1
- throughput: float32 [4, 5120], P(None, 'fiber'), may hold values from 0.5 to 1.5
Outputs:
- residual: float32 [4, 5120, 8192], P(None, 'fiber', 'wave')
- chi_square: float32 [4, 5120], P(None, 'fiber')
- sky_coeffs: float32 [16, 8192], P(None, 'wave')
The draws below stay inside these ranges and needn't reach their ends.
Inputs may be any that keep to these rules, and one draw needn't show every extreme that they name: `mask_bits`: each entry is zero or one single bit of 0 to 9. `fiber_ids`: each fiber id appears in exactly one slot.
All inputs are finite; a program needn't handle non-finite values. No bound on the sum of `sky_flags` on one device may be relied on, other than what follows from the above.
Results may differ from the reference program's by a relative error of at most 0.0003.
Values sent between devices are 32-bit elements; how exact they have to be, the bound alone decides.
No kernel may reach another device: no remote copies, remote signals or barrier semaphores. Data moves between devices by JAX's collectives and lax.ppermute only.
A program may use at most 64 MiB of HBM per device.

```python
import math
import jax
import jax.numpy as jnp
from jax import lax

E = 4
PARAMS = 16
FIBERS = 5120
WAVES = 8192


def draw_mask_bits(key, part):
    raw = jax.random.randint(key, (E, FIBERS, WAVES), 0, 64)
    flagged = jnp.left_shift(jnp.ones_like(raw), raw % 10)
    return jnp.where(raw < 20, flagged, 0).astype(jnp.int32)


def set_ends(drawn, key, smallest, high):
    index_at = [jax.random.randint(jax.random.fold_in(key, axis), (), 0, length) for axis, length in enumerate(drawn.shape)]
    main_axis = drawn.shape.index(max(drawn.shape))
    beside = index_at[:main_axis] + [(index_at[main_axis] + 1) % drawn.shape[main_axis]] + index_at[main_axis + 1:]
    return drawn.at[tuple(index_at)].set(smallest).at[tuple(beside)].set(high)


def shard_levels(rng, dims, pieces, least, top_value):
    factor_of = 1.0
    for dim, shards_of in pieces:
        heights = jax.random.uniform(jax.random.fold_in(jax.random.fold_in(rng, 6), dim), (shards_of,), jnp.float32, least / len(pieces), top_value / len(pieces))
        factor_of = factor_of * jnp.repeat(jnp.exp(heights), dims[dim] // shards_of).reshape((-1,) + (1,) * (len(dims) - 1 - dim))
    return factor_of


def setup_inputs(seed: int = 0) -> dict:
    key_list = jax.random.split(jax.random.key(seed), 8)
    return {
        "spectra": jnp.clip(10.0 * jax.random.uniform(key_list[0], (E, FIBERS, WAVES), jnp.float32) ** shard_levels(key_list[0], (E, FIBERS, WAVES), ((1, 128), (2, 2)), -0.2, 0.2), 0.0, 10.0),
        "inverse_var": jnp.clip(jnp.exp(math.log(10.0) - 4.6051702 * jax.random.uniform(key_list[1], (E, FIBERS, WAVES), jnp.float32) ** shard_levels(key_list[1], (E, FIBERS, WAVES), ((1, 128), (2, 2)), -0.2, 0.2)), 0.1, 10.0),
        "mask_bits": draw_mask_bits(jax.random.fold_in(key_list[7], 71), 0),
        "sky_flags": set_ends((jax.random.randint(key_list[3], (E, FIBERS), 0, 8) < 1).astype(jnp.int32), jax.random.fold_in(key_list[3], 1), 0, 1),
        "fiber_ids": jax.random.permutation(key_list[4], FIBERS).astype(jnp.int32),
        "positions": jnp.clip(jax.random.uniform(key_list[5], (2, FIBERS), jnp.float32, -1.0, 1.0), -1.0, 1.0),
        "throughput": jnp.clip(1.0 + 0.1 * jax.random.normal(key_list[6], (E, FIBERS), jnp.float32), 0.5, 1.5),
    }


bad_bits = 31
prior_weight = 1.0
highest = lax.Precision.HIGHEST

def legendre(coord):
    return [jnp.ones_like(coord), coord, 1.5 * coord * coord - 0.5, (2.5 * coord * coord - 1.5) * coord]

def build_design(positions, fiber_ids, throughput):
    coord_x = positions[0][fiber_ids]
    coord_y = positions[1][fiber_ids]
    poly_x = legendre(coord_x)
    poly_y = legendre(coord_y)
    basis = jnp.stack([along_x * along_y for along_x in poly_x for along_y in poly_y], axis=-1)
    return throughput[:, :, None] * basis[None]

def solve_normal(matrix, right_side):
    param_count = right_side.shape[0]
    factor = {}
    for column in range(param_count):
        pivot_sum = matrix[column * param_count + column] + prior_weight
        for inner_k in range(column):
            pivot_sum = pivot_sum - factor[column, inner_k] * factor[column, inner_k]
        root_value = jnp.sqrt(pivot_sum)
        factor[column, column] = root_value
        for target in range(column + 1, param_count):
            running = matrix[target * param_count + column]
            for inner_k in range(column):
                running = running - factor[target, inner_k] * factor[column, inner_k]
            factor[target, column] = running / root_value
    interim = []
    for target in range(param_count):
        running = right_side[target]
        for inner_k in range(target):
            running = running - factor[target, inner_k] * interim[inner_k]
        interim.append(running / factor[target, target])
    solved = [None] * param_count
    for target in reversed(range(param_count)):
        running = interim[target]
        for inner_k in range(target + 1, param_count):
            running = running - factor[inner_k, target] * solved[inner_k]
        solved[target] = running / factor[target, target]
    return jnp.stack(solved)

def reference(spectra, inverse_var, mask_bits, sky_flags, fiber_ids, positions, throughput):
    row_count = E * FIBERS
    design = build_design(positions, fiber_ids, throughput).reshape(row_count, PARAMS)
    products = (design[:, :, None] * design[:, None, :]).reshape(row_count, PARAMS * PARAMS)
    sky_rows = sky_flags.reshape(row_count).astype(jnp.float32)
    block_width = 512 if WAVES % 512 == 0 else 128

    def step_fn(index, carry):
        residual_all, coeff_all, chi_sum = carry
        offset = (index * block_width).astype(jnp.int32)
        flux_block = lax.dynamic_slice_in_dim(spectra, offset, block_width, 2).reshape(row_count, block_width)
        ivar_block = lax.dynamic_slice_in_dim(inverse_var, offset, block_width, 2).reshape(row_count, block_width)
        bits_block = lax.dynamic_slice_in_dim(mask_bits, offset, block_width, 2).reshape(row_count, block_width)
        usable = (bits_block & bad_bits == 0).astype(jnp.float32)
        noise_weight = ivar_block * usable
        fit_weights = noise_weight * sky_rows[:, None]
        normal = jnp.dot(products.T, fit_weights, precision=highest)
        right_side = jnp.dot(design.T, fit_weights * flux_block, precision=highest)
        block_coeffs = solve_normal(normal, right_side)
        residual = flux_block - jnp.dot(design, block_coeffs, precision=highest)
        chi_sum = chi_sum + lax.optimization_barrier(jnp.sum(noise_weight * residual * residual, axis=1))
        residual_all = lax.dynamic_update_slice_in_dim(residual_all, residual.reshape(E, FIBERS, block_width), offset, 2)
        coeff_all = lax.dynamic_update_slice_in_dim(coeff_all, block_coeffs, offset, 1)
        return (residual_all, coeff_all, chi_sum)
    start_state = (jnp.zeros((E, FIBERS, WAVES), jnp.float32), jnp.zeros((PARAMS, WAVES), jnp.float32), jnp.zeros((row_count,), jnp.float32))
    residual_all, coeff_all, chi_sum = lax.fori_loop(0, WAVES // block_width, step_fn, start_state)
    chi_square = (chi_sum / WAVES).reshape(E, FIBERS)
    return (residual_all, chi_square, coeff_all)
```

```python
import functools

import jax
import jax.numpy as jnp
from jax import lax
from jax.experimental import pallas as pl
from jax.experimental.pallas import tpu as pltpu
from jax.sharding import PartitionSpec as P

PARAMS = 16
BAD_BITS = 31
PRIOR = 1.0
MOMENTS = 7
BASIS = 4
RIGHT_ROW = 56
PACKED = 72
LANES = 128
BLOCK = 512


def legendre_series(coord, total):
    series = [jnp.ones_like(coord), coord]
    for order in range(1, total - 1):
        series.append(((2 * order + 1) * coord * series[order] - order * series[order - 1]) / (order + 1))
    return series


def monomial_table(total):
    coeffs = [[0.0] * total for _ in range(total)]
    coeffs[0][0] = 1.0
    coeffs[1][1] = 1.0
    for order in range(1, total - 1):
        for power in range(total):
            raised = coeffs[order][power - 1] if power >= 1 else 0.0
            coeffs[order + 1][power] = ((2 * order + 1) * raised - order * coeffs[order - 1][power]) / (order + 1)
    return coeffs


def product_series(higher, first, second):
    product = [0.0] * MOMENTS
    for left in range(MOMENTS):
        for right in range(MOMENTS - left):
            product[left + right] += higher[first][left] * higher[second][right]
    series = [0.0] * MOMENTS
    for order in reversed(range(MOMENTS)):
        now = product[order] / higher[order][order]
        series[order] = now
        for power in range(MOMENTS):
            product[power] -= now * higher[order][power]
    return series


def rebuild_rows():
    higher = monomial_table(MOMENTS)
    pair = [[product_series(higher, a, b) for b in range(BASIS)] for a in range(BASIS)]
    rows = []
    for i in range(BASIS):
        for j in range(BASIS):
            for k in range(BASIS):
                for l in range(BASIS):
                    row = [0.0] * LANES
                    for a in range(MOMENTS):
                        for b in range(MOMENTS):
                            row[a * MOMENTS + b] = pair[i][k][a] * pair[j][l][b]
                    rows.append(row)
    return rows


def split3(value):
    high = value.astype(jnp.bfloat16)
    rest = value - high.astype(jnp.float32)
    middle = rest.astype(jnp.bfloat16)
    low = (rest - middle.astype(jnp.float32)).astype(jnp.bfloat16)
    return high, middle, low


def dot6(left, right):
    l1, l2, l3 = split3(left)
    r1, r2, r3 = split3(right)
    total = None
    for a, b in ((l1, r3), (l3, r1), (l2, r2), (l1, r2), (l2, r1), (l1, r1)):
        part = jnp.dot(a, b, preferred_element_type=jnp.float32)
        total = part if total is None else total + part
    return total


def moments_kernel(ids_ref, pos_ref, tput_ref, sky_ref, flux_ref, ivar_ref, bits_ref, out_ref, feat_ref, small_ref, stack_ref, left_ref):
    fibers = flux_ref.shape[1]
    exposures = flux_ref.shape[0]

    @pl.when(pl.program_id(0) == 0)
    def _():
        stack_ref[...] = jnp.zeros_like(stack_ref)
        stack_ref[0:exposures, 0:fibers] = tput_ref[...]
        stack_ref[8:8 + exposures, 0:fibers] = sky_ref[...].astype(jnp.float32)
        turned = stack_ref[0:LANES, :].T
        sub = lax.broadcasted_iota(jnp.int32, (fibers, LANES), 0)
        lane = lax.broadcasted_iota(jnp.int32, (fibers, LANES), 1)
        ids = jnp.zeros((fibers, LANES), jnp.int32)
        for f in range(fibers):
            ids = jnp.where(sub == f, ids_ref[f], ids)
        sum_x = jnp.zeros((fibers, LANES), jnp.float32)
        sum_y = jnp.zeros((fibers, LANES), jnp.float32)
        offset = ids - lane
        for tile in range(pos_ref.shape[1] // LANES):
            hit = offset == tile * LANES
            cut = slice(tile * LANES, (tile + 1) * LANES)
            sum_x = jnp.where(hit, pos_ref[0:1, cut], sum_x)
            sum_y = jnp.where(hit, pos_ref[1:2, cut], sum_y)
        coord_x = jnp.sum(sum_x, axis=1, keepdims=True)
        coord_y = jnp.sum(sum_y, axis=1, keepdims=True)
        series_x = legendre_series(jnp.broadcast_to(coord_x, (fibers, LANES)), MOMENTS)
        series_y = legendre_series(jnp.broadcast_to(coord_y, (fibers, LANES)), MOMENTS)
        is_right = lane >= RIGHT_ROW
        index_x = jnp.where(is_right, (lane - RIGHT_ROW) // BASIS, lane // MOMENTS)
        index_y = jnp.where(is_right, (lane - RIGHT_ROW) % BASIS, lane % MOMENTS)
        along_x = jnp.zeros((fibers, LANES), jnp.float32)
        along_y = jnp.zeros((fibers, LANES), jnp.float32)
        for order in range(MOMENTS):
            along_x = jnp.where(index_x == order, series_x[order], along_x)
            along_y = jnp.where(index_y == order, series_y[order], along_y)
        product = along_x * along_y
        moment_part = jnp.where(lane < MOMENTS * MOMENTS, product, 0.0)
        right_part = jnp.where(is_right & (lane < RIGHT_ROW + PARAMS), product, 0.0)
        feat_ref[0:fibers, :] = right_part
        feat_ref[fibers:2 * fibers, :] = turned[0:fibers, :]
        small_ref[...] = turned[0:fibers, :]
        both = jnp.concatenate([moment_part, right_part], axis=0)
        high, middle, low = (part.astype(jnp.float32) for part in split3(both))
        rows = 2 * fibers
        for place, part in enumerate((high, middle, low, high, middle, high)):
            stack_ref[place * rows:(place + 1) * rows, :] = part
        stack_ref[6 * rows:, :] = jnp.zeros((stack_ref.shape[0] - 6 * rows, LANES), jnp.float32)
        for tile in range(stack_ref.shape[0] // LANES):
            cut = slice(tile * LANES, (tile + 1) * LANES)
            left_ref[:, cut] = stack_ref[cut, :].T[0:left_ref.shape[0], :].astype(jnp.bfloat16)

    columns = small_ref[...]
    moment_rows = None
    right_rows = None
    for e in range(exposures):
        through = columns[:, e:e + 1]
        sky = columns[:, 8 + e:9 + e]
        weight = jnp.where((bits_ref[e] & BAD_BITS) == 0, ivar_ref[e], 0.0)
        first = weight * (through * sky)
        a = first * through
        b = first * flux_ref[e]
        moment_rows = a if e == 0 else moment_rows + a
        right_rows = b if e == 0 else right_rows + b
    high, middle, low = split3(jnp.concatenate([moment_rows, right_rows], axis=0))
    right = jnp.concatenate([high, high, high, middle, middle, low], axis=0)
    sums = jnp.dot(left_ref[:, 0:right.shape[0]], right, preferred_element_type=jnp.float32)
    for k in range(out_ref.shape[0]):
        out_ref[k] = sums[0:PACKED, k * LANES:(k + 1) * LANES]


def add_kernel(in_ref, out_ref):
    total = in_ref[0]
    for source in range(1, in_ref.shape[0]):
        total = total + in_ref[source]
    for target in range(out_ref.shape[0]):
        out_ref[target] = total


def solve_kernel(in_ref, table_ref, out_ref):
    total = in_ref[0]
    for source in range(1, in_ref.shape[0]):
        total = total + in_ref[source]
    moments = jnp.concatenate([total[0:RIGHT_ROW], jnp.zeros((LANES - RIGHT_ROW, LANES), jnp.float32)], axis=0)
    normal = dot6(table_ref[...], moments)
    sub = lax.broadcasted_iota(jnp.int32, (PARAMS, LANES), 0)
    columns = []
    for k in range(PARAMS):
        column = normal[k * PARAMS:(k + 1) * PARAMS]
        columns.append(jnp.where(sub == k, column + PRIOR, column))
    right = total[RIGHT_ROW:RIGHT_ROW + PARAMS]
    scale = jnp.zeros((PARAMS, LANES), jnp.float32)
    for j in range(PARAMS):
        inverse = 1.0 / columns[j][j:j + 1]
        scale = jnp.where(sub == j, inverse, scale)
        factor = jnp.where(sub == j, 0.0, columns[j] * inverse)
        for l in range(j + 1, PARAMS):
            columns[l] = columns[l] - factor * columns[l][j:j + 1]
        right = right - factor * right[j:j + 1]
    right = right * scale
    for target in range(out_ref.shape[0]):
        out_ref[target] = right


def residual_kernel(feat_ref, coeff_ref, flux_ref, ivar_ref, bits_ref, res_ref, all_ref, chi_ref, sum_ref):
    step = pl.program_id(0)
    exposures, fibers, width = flux_ref.shape

    @pl.when(step == 0)
    def _():
        sum_ref[...] = jnp.zeros_like(sum_ref)

    coeffs = jnp.concatenate([coeff_ref[k] for k in range(coeff_ref.shape[0])], axis=1)
    all_ref[...] = coeffs
    basis = feat_ref[0:fibers, RIGHT_ROW:RIGHT_ROW + PARAMS]
    model = dot6(basis, coeffs)
    for e in range(exposures):
        through = feat_ref[fibers:2 * fibers, e:e + 1]
        residual = flux_ref[e] - through * model
        res_ref[e] = residual
        weight = jnp.where((bits_ref[e] & BAD_BITS) == 0, ivar_ref[e], 0.0)
        chi = weight * residual * residual
        part = chi[:, 0:LANES]
        for k in range(1, width // LANES):
            part = part + chi[:, k * LANES:(k + 1) * LANES]
        sum_ref[e * fibers:(e + 1) * fibers, :] += part

    @pl.when(step == pl.num_programs(0) - 1)
    def _():
        ones = jnp.ones((8, LANES), jnp.float32)
        chi_ref[...] = lax.dot_general(ones, sum_ref[...], (((1,), (1,)), ((), ())), precision=lax.Precision.HIGHEST, preferred_element_type=jnp.float32)


def chi_kernel(scale, mine_ref, other_ref, out_ref):
    exposures, fibers = out_ref.shape
    total = (mine_ref[...] + other_ref[...]) * scale
    for e in range(exposures):
        out_ref[e:e + 1, :] = total[0:1, e * fibers:(e + 1) * fibers]


def vmem(*shape):
    return pl.BlockSpec(shape, lambda *_: (0,) * len(shape))


def cost(flops, moved):
    return pl.CostEstimate(flops=flops, bytes_accessed=moved, transcendentals=0)


def params(limit_mib, dims=0):
    semantics = {"dimension_semantics": ("arbitrary",) * dims} if dims else {}
    return pltpu.CompilerParams(vmem_limit_bytes=limit_mib * 1024 * 1024, **semantics)


def groups(sizes):
    nz, ny, nx = sizes

    def place(z, y, x):
        return (z * ny + y) * nx + x

    pair = 2
    near = [[place(q * pair + h, y, x) for h in range(pair) for y in range(ny) for x in range(nx)] for q in range(nz // pair)]
    far = [[place(q * pair + h, y, x) for q in range(nz // pair)] for h in range(pair) for y in range(ny) for x in range(nx)]
    return near, far


def make_body(near, far):
    def body(spectra, inverse_var, mask_bits, sky_flags, fiber_ids, positions, throughput):
        exposures, fibers, waves = spectra.shape
        steps = waves // BLOCK
        per_step = BLOCK // LANES
        f32 = jnp.float32
        wide = pl.BlockSpec((exposures, fibers, BLOCK), lambda s: (0, 0, s))
        stacked = -(-12 * fibers // LANES) * LANES

        packed, feats = pl.pallas_call(
            moments_kernel,
            grid=(steps,),
            in_specs=[
                pl.BlockSpec(memory_space=pltpu.SMEM),
                vmem(*positions.shape),
                vmem(exposures, fibers),
                vmem(exposures, fibers),
                wide, wide, wide,
            ],
            out_specs=[
                pl.BlockSpec((per_step, PACKED, LANES), lambda s: (s, 0, 0)),
                vmem(2 * fibers, LANES),
            ],
            out_shape=[
                jax.ShapeDtypeStruct((waves // LANES, PACKED, LANES), f32),
                jax.ShapeDtypeStruct((2 * fibers, LANES), f32),
            ],
            scratch_shapes=[
                pltpu.VMEM((fibers, LANES), f32),
                pltpu.VMEM((stacked, LANES), f32),
                pltpu.VMEM((80, stacked), jnp.bfloat16),
            ],
            compiler_params=params(16, 1),
            cost_estimate=cost(2 * 6 * PACKED * 2 * fibers * waves, 3 * 4 * exposures * fibers * waves),
            name="moments",
        )(fiber_ids, positions, throughput, sky_flags, spectra, inverse_var, mask_bits)

        arrived = lax.all_to_all(packed, "fiber", 0, 0, axis_index_groups=near, tiled=True)
        copies = pl.pallas_call(
            add_kernel,
            out_shape=jax.ShapeDtypeStruct((len(far[0]), PACKED, LANES), f32),
            compiler_params=params(8),
            name="add",
        )(arrived)
        parts = lax.all_to_all(copies, "fiber", 0, 0, axis_index_groups=far, tiled=True)
        solved = pl.pallas_call(
            solve_kernel,
            out_shape=jax.ShapeDtypeStruct((len(near[0]), PARAMS, LANES), f32),
            compiler_params=params(8),
            name="solve",
        )(parts, jnp.asarray(rebuild_rows(), f32))
        coeffs = lax.all_to_all(solved, "fiber", 0, 0, axis_index_groups=near, tiled=True)

        residual, sky_coeffs, chi_local = pl.pallas_call(
            residual_kernel,
            grid=(steps,),
            in_specs=[
                vmem(2 * fibers, LANES),
                pl.BlockSpec((per_step, PARAMS, LANES), lambda s: (s, 0, 0)),
                wide, wide, wide,
            ],
            out_specs=[
                wide,
                pl.BlockSpec((PARAMS, BLOCK), lambda s: (0, s)),
                vmem(8, exposures * fibers),
            ],
            out_shape=[
                jax.ShapeDtypeStruct(spectra.shape, f32),
                jax.ShapeDtypeStruct((PARAMS, waves), f32),
                jax.ShapeDtypeStruct((8, exposures * fibers), f32),
            ],
            scratch_shapes=[pltpu.VMEM((exposures * fibers, LANES), f32)],
            compiler_params=params(16, 1),
            cost_estimate=cost(2 * 6 * PARAMS * fibers * waves, 4 * 4 * exposures * fibers * waves),
            name="residual",
        )(feats, coeffs, spectra, inverse_var, mask_bits)

        halves = lax.axis_size("wave")
        chi_other = lax.ppermute(chi_local, "wave", [(h, (h + 1) % halves) for h in range(halves)])
        chi_square = pl.pallas_call(
            functools.partial(chi_kernel, 1.0 / (waves * halves)),
            out_shape=jax.ShapeDtypeStruct((exposures, fibers), f32),
            compiler_params=params(4),
            name="chi",
        )(chi_local, chi_other)
        return residual, chi_square, sky_coeffs

    return body


def solution(mesh):
    near, far = groups((8, 4, 4))
    placed = (
        P(None, "fiber", "wave"),
        P(None, "fiber", "wave"),
        P(None, "fiber", "wave"),
        P(None, "fiber"),
        P("fiber"),
        P(),
        P(None, "fiber"),
    )
    return jax.shard_map(
        make_body(near, far),
        mesh=mesh,
        in_specs=placed,
        out_specs=(P(None, "fiber", "wave"), P(None, "fiber"), P(None, "wave")),
        check_vma=False,
    )
```

```python
import functools

import jax
import jax.numpy as jnp
from jax import lax
from jax.experimental import pallas as pl
from jax.experimental.pallas import tpu as pltpu
from jax.sharding import PartitionSpec as P

PARAMS = 16
BAD_BITS = 31
PRIOR = 1.0
MOMENTS = 7
BASIS = 4
RIGHT_ROW = 56
PACKED = 72
LANES = 128
PIECE = 512
FLOPS = 4_000_000_000


def legendre_series(coord, total):
    series = [jnp.ones_like(coord), coord]
    for order in range(1, total - 1):
        series.append(((2 * order + 1) * coord * series[order] - order * series[order - 1]) / (order + 1))
    return series


def monomial_table(total):
    coeffs = [[0.0] * total for _ in range(total)]
    coeffs[0][0] = 1.0
    coeffs[1][1] = 1.0
    for order in range(1, total - 1):
        for power in range(total):
            raised = coeffs[order][power - 1] if power >= 1 else 0.0
            coeffs[order + 1][power] = ((2 * order + 1) * raised - order * coeffs[order - 1][power]) / (order + 1)
    return coeffs


def product_series(higher, first, second):
    product = [0.0] * MOMENTS
    for left in range(MOMENTS):
        for right in range(MOMENTS - left):
            product[left + right] += higher[first][left] * higher[second][right]
    series = [0.0] * MOMENTS
    for order in reversed(range(MOMENTS)):
        now = product[order] / higher[order][order]
        series[order] = now
        for power in range(MOMENTS):
            product[power] -= now * higher[order][power]
    return series


def rebuild_rows():
    higher = monomial_table(MOMENTS)
    pair = [[product_series(higher, a, b) for b in range(BASIS)] for a in range(BASIS)]
    rows = []
    for i in range(BASIS):
        for j in range(BASIS):
            for k in range(BASIS):
                for l in range(BASIS):
                    row = [0.0] * LANES
                    for a in range(MOMENTS):
                        for b in range(MOMENTS):
                            row[a * MOMENTS + b] = pair[i][k][a] * pair[j][l][b]
                    rows.append(row)
    return rows


def split3(value):
    high = value.astype(jnp.bfloat16)
    rest = value - high.astype(jnp.float32)
    middle = rest.astype(jnp.bfloat16)
    low = (rest - middle.astype(jnp.float32)).astype(jnp.bfloat16)
    return high, middle, low


def dot6(left, right):
    l1, l2, l3 = split3(left)
    r1, r2, r3 = split3(right)
    total = None
    for a, b in ((l1, r3), (l3, r1), (l2, r2), (l1, r2), (l2, r1), (l1, r1)):
        part = jnp.dot(a, b, preferred_element_type=jnp.float32)
        total = part if total is None else total + part
    return total


def build_features(ids_ref, pos_ref, tput_ref, sky_ref, stack_ref, feat_ref, left_ref):
    exposures, fibers = tput_ref.shape
    stack_ref[0:LANES, :] = jnp.zeros((LANES, LANES), jnp.float32)
    stack_ref[0:exposures, 0:fibers] = tput_ref[...]
    stack_ref[8:8 + exposures, 0:fibers] = sky_ref[...].astype(jnp.float32)
    stack_ref[16:17, 0:fibers] = ids_ref[...].reshape(1, fibers).astype(jnp.float32)
    turned = stack_ref[0:LANES, :].T
    lane = lax.broadcasted_iota(jnp.int32, (fibers, LANES), 1)
    ids = jnp.broadcast_to(turned[0:fibers, 16:17], (fibers, LANES)).astype(jnp.int32)
    sum_x = jnp.zeros((fibers, LANES), jnp.float32)
    sum_y = jnp.zeros((fibers, LANES), jnp.float32)
    offset = ids - lane
    for tile in range(pos_ref.shape[1] // LANES):
        hit = offset == tile * LANES
        cut = slice(tile * LANES, (tile + 1) * LANES)
        sum_x = jnp.where(hit, pos_ref[0:1, cut], sum_x)
        sum_y = jnp.where(hit, pos_ref[1:2, cut], sum_y)
    coord_x = jnp.sum(sum_x, axis=1, keepdims=True)
    coord_y = jnp.sum(sum_y, axis=1, keepdims=True)
    series_x = legendre_series(jnp.broadcast_to(coord_x, (fibers, LANES)), MOMENTS)
    series_y = legendre_series(jnp.broadcast_to(coord_y, (fibers, LANES)), MOMENTS)
    is_right = lane >= RIGHT_ROW
    index_x = jnp.where(is_right, (lane - RIGHT_ROW) // BASIS, lane // MOMENTS)
    index_y = jnp.where(is_right, (lane - RIGHT_ROW) % BASIS, lane % MOMENTS)
    along_x = jnp.zeros((fibers, LANES), jnp.float32)
    along_y = jnp.zeros((fibers, LANES), jnp.float32)
    for order in range(MOMENTS):
        along_x = jnp.where(index_x == order, series_x[order], along_x)
        along_y = jnp.where(index_y == order, series_y[order], along_y)
    product = along_x * along_y
    moment_part = jnp.where(lane < MOMENTS * MOMENTS, product, 0.0)
    right_part = jnp.where(is_right & (lane < RIGHT_ROW + PARAMS), product, 0.0)
    feat_ref[0:fibers, :] = right_part
    feat_ref[fibers:2 * fibers, :] = turned[0:fibers, :]
    both = jnp.concatenate([moment_part, right_part], axis=0)
    high, middle, low = (part.astype(jnp.float32) for part in split3(both))
    rows = 2 * fibers
    for place, part in enumerate((high, middle, low, high, middle, high)):
        stack_ref[place * rows:(place + 1) * rows, :] = part
    stack_ref[6 * rows:, :] = jnp.zeros((stack_ref.shape[0] - 6 * rows, LANES), jnp.float32)
    for tile in range(stack_ref.shape[0] // LANES):
        cut = slice(tile * LANES, (tile + 1) * LANES)
        left_ref[:, cut] = stack_ref[cut, :].T[0:left_ref.shape[0], :].astype(jnp.bfloat16)


def piece_copies(flux_hbm, ivar_hbm, bits_hbm, flux_ref, ivar_ref, bits_ref, sems):
    copies = []
    for piece in range(flux_ref.shape[2] // PIECE):
        cut = pl.ds(piece * PIECE, PIECE)
        copies.append([
            pltpu.make_async_copy(source.at[:, :, cut], target.at[:, :, cut], sems.at[piece, which])
            for which, (source, target) in enumerate(((flux_hbm, flux_ref), (ivar_hbm, ivar_ref), (bits_hbm, bits_ref)))
        ])
    return copies


def sum_pieces(copies, feat_ref, left_ref, flux_ref, ivar_ref, bits_ref, out_ref, weight_ref):
    exposures, fibers, _ = flux_ref.shape
    columns = feat_ref[fibers:2 * fibers, :]
    for piece, trio in enumerate(copies):
        for copy in trio:
            copy.wait()
        here = slice(piece * PIECE, (piece + 1) * PIECE)
        moment_rows = None
        right_rows = None
        for e in range(exposures):
            through = columns[:, e:e + 1]
            sky = columns[:, 8 + e:9 + e]
            weight = jnp.where((bits_ref[e, :, here] & BAD_BITS) == 0, ivar_ref[e, :, here], 0.0)
            weight_ref[e, :, here] = weight
            first = weight * (through * sky)
            a = first * through
            b = first * flux_ref[e, :, here]
            moment_rows = a if e == 0 else moment_rows + a
            right_rows = b if e == 0 else right_rows + b
        high, middle, low = split3(jnp.concatenate([moment_rows, right_rows], axis=0))
        right = jnp.concatenate([high, high, high, middle, middle, low], axis=0)
        sums = jnp.dot(left_ref[:, 0:right.shape[0]], right, preferred_element_type=jnp.float32)
        for k in range(PIECE // LANES):
            out_ref[piece * (PIECE // LANES) + k] = sums[0:PACKED, k * LANES:(k + 1) * LANES]


def moments_kernel(ids_hbm, pos_hbm, tput_hbm, sky_hbm, flux_hbm, ivar_hbm, bits_hbm, out_ref, feat_ref, flux_ref, weight_ref,
                   ids_ref, pos_ref, tput_ref, sky_ref, ivar_ref, bits_ref, left_ref, stack_ref, small_sems, sems):
    small = [
        pltpu.make_async_copy(source, target, small_sems.at[place])
        for place, (source, target) in enumerate(((ids_hbm, ids_ref), (pos_hbm, pos_ref), (tput_hbm, tput_ref), (sky_hbm, sky_ref)))
    ]
    for copy in small:
        copy.start()
    copies = piece_copies(flux_hbm, ivar_hbm, bits_hbm, flux_ref, ivar_ref, bits_ref, sems)
    for trio in copies:
        for copy in trio:
            copy.start()
    for copy in small:
        copy.wait()
    build_features(ids_ref, pos_ref, tput_ref, sky_ref, stack_ref, feat_ref, left_ref)
    sum_pieces(copies, feat_ref, left_ref, flux_ref, ivar_ref, bits_ref, out_ref, weight_ref)


def add_kernel(in_ref, out_ref):
    total = in_ref[0]
    for source in range(1, in_ref.shape[0]):
        total = total + in_ref[source]
    for target in range(out_ref.shape[0]):
        out_ref[target] = total


def solve_kernel(in_ref, table_ref, out_ref):
    total = in_ref[0]
    for source in range(1, in_ref.shape[0]):
        total = total + in_ref[source]
    moments = jnp.concatenate([total[0:RIGHT_ROW], jnp.zeros((LANES - RIGHT_ROW, LANES), jnp.float32)], axis=0)
    normal = dot6(table_ref[...], moments)
    sub = lax.broadcasted_iota(jnp.int32, (PARAMS, LANES), 0)
    columns = []
    for k in range(PARAMS):
        column = normal[k * PARAMS:(k + 1) * PARAMS]
        columns.append(jnp.where(sub == k, column + PRIOR, column))
    right = total[RIGHT_ROW:RIGHT_ROW + PARAMS]
    scale = jnp.zeros((PARAMS, LANES), jnp.float32)
    for j in range(PARAMS):
        inverse = 1.0 / columns[j][j:j + 1]
        scale = jnp.where(sub == j, inverse, scale)
        factor = jnp.where(sub == j, 0.0, columns[j] * inverse)
        for l in range(j + 1, PARAMS):
            columns[l] = columns[l] - factor * columns[l][j:j + 1]
        right = right - factor * right[j:j + 1]
    right = right * scale
    for target in range(out_ref.shape[0]):
        out_ref[target] = right


def joined(coeff_ref, first, count):
    return jnp.concatenate([coeff_ref[first + k] for k in range(count)], axis=1)


def chi_sum_kernel(feat_ref, coeff_ref, flux_ref, weight_ref, chi_ref, sum_ref):
    exposures, fibers, waves = flux_ref.shape
    basis = feat_ref[0:fibers, RIGHT_ROW:RIGHT_ROW + PARAMS]
    sums = [None] * exposures
    for piece in range(waves // PIECE):
        here = slice(piece * PIECE, (piece + 1) * PIECE)
        model = dot6(basis, joined(coeff_ref, piece * (PIECE // LANES), PIECE // LANES))
        for e in range(exposures):
            residual = flux_ref[e, :, here] - feat_ref[fibers:2 * fibers, e:e + 1] * model
            chi = weight_ref[e, :, here] * residual * residual
            for k in range(PIECE // LANES):
                part = chi[:, k * LANES:(k + 1) * LANES]
                sums[e] = part if sums[e] is None else sums[e] + part
    for e in range(exposures):
        sum_ref[e * fibers:(e + 1) * fibers, :] = sums[e]
    ones = jnp.ones((8, LANES), jnp.float32)
    chi_ref[...] = lax.dot_general(ones, sum_ref[...], (((1,), (1,)), ((), ())), precision=lax.Precision.HIGHEST, preferred_element_type=jnp.float32)


def write_kernel(feat_ref, coeff_ref, flux_ref, res_hbm, all_hbm, res_ref, all_ref, sems, all_sem):
    exposures, fibers, waves = flux_ref.shape
    basis = feat_ref[0:fibers, RIGHT_ROW:RIGHT_ROW + PARAMS]
    copies = []
    for piece in range(waves // PIECE):
        here = slice(piece * PIECE, (piece + 1) * PIECE)
        coeffs = joined(coeff_ref, piece * (PIECE // LANES), PIECE // LANES)
        all_ref[:, here] = coeffs
        model = dot6(basis, coeffs)
        for e in range(exposures):
            res_ref[e, :, here] = flux_ref[e, :, here] - feat_ref[fibers:2 * fibers, e:e + 1] * model
        cut = pl.ds(piece * PIECE, PIECE)
        copies.append(pltpu.make_async_copy(res_ref.at[:, :, cut], res_hbm.at[:, :, cut], sems.at[piece]))
        copies[-1].start()
    copies.append(pltpu.make_async_copy(all_ref, all_hbm, all_sem))
    copies[-1].start()
    for copy in copies:
        copy.wait()


def chi_kernel(scale, mine_ref, other_ref, out_ref):
    exposures, fibers = out_ref.shape
    total = (mine_ref[...] + other_ref[...]) * scale
    for e in range(exposures):
        out_ref[e:e + 1, :] = total[0:1, e * fibers:(e + 1) * fibers]


def cost(flops, moved):
    return pl.CostEstimate(flops=flops, bytes_accessed=moved, transcendentals=0)


def params(limit_mib, dims=0):
    semantics = {"dimension_semantics": ("arbitrary",) * dims} if dims else {}
    return pltpu.CompilerParams(vmem_limit_bytes=limit_mib * 1024 * 1024, **semantics)


def groups(sizes):
    nz, ny, nx = sizes

    def place(z, y, x):
        return (z * ny + y) * nx + x

    pair = 2
    near = [[place(q * pair + h, y, x) for h in range(pair) for y in range(ny) for x in range(nx)] for q in range(nz // pair)]
    far = [[place(q * pair + h, y, x) for q in range(nz // pair)] for h in range(pair) for y in range(ny) for x in range(nx)]
    return near, far


VMEM = pl.BlockSpec(memory_space=pltpu.VMEM)
HBM = pl.BlockSpec(memory_space=pltpu.HBM)


def make_body(near, far):
    def body(spectra, inverse_var, mask_bits, sky_flags, fiber_ids, positions, throughput):
        exposures, fibers, waves = spectra.shape
        f32 = jnp.float32
        pieces = waves // PIECE
        stacked = -(-12 * fibers // LANES) * LANES
        moved = 4 * exposures * fibers * waves

        held = [
            pltpu.with_memory_space_constraint(value, pltpu.HBM)
            for value in (fiber_ids, positions, throughput, sky_flags, spectra, inverse_var, mask_bits)
        ]
        packed, feats, flux, weight = pl.pallas_call(
            moments_kernel,
            in_specs=[HBM] * 7,
            out_specs=[VMEM] * 4,
            out_shape=[
                jax.ShapeDtypeStruct((waves // LANES, PACKED, LANES), f32),
                jax.ShapeDtypeStruct((2 * fibers, LANES), f32),
                jax.ShapeDtypeStruct(spectra.shape, f32),
                jax.ShapeDtypeStruct(spectra.shape, f32),
            ],
            scratch_shapes=[
                pltpu.VMEM(fiber_ids.shape, jnp.int32),
                pltpu.VMEM(positions.shape, f32),
                pltpu.VMEM((exposures, fibers), f32),
                pltpu.VMEM((exposures, fibers), jnp.int32),
                pltpu.VMEM(spectra.shape, f32),
                pltpu.VMEM(spectra.shape, jnp.int32),
                pltpu.VMEM((80, stacked), jnp.bfloat16),
                pltpu.VMEM((stacked, LANES), f32),
                pltpu.SemaphoreType.DMA((4,)),
                pltpu.SemaphoreType.DMA((pieces, 3)),
            ],
            compiler_params=params(20),
            cost_estimate=cost(FLOPS, 3 * moved),
            name="moments",
        )(*held)

        arrived = lax.all_to_all(packed, "fiber", 0, 0, axis_index_groups=near, tiled=True)
        copies = pl.pallas_call(
            add_kernel,
            out_shape=jax.ShapeDtypeStruct((len(far[0]), PACKED, LANES), f32),
            compiler_params=params(8),
            name="add",
        )(arrived)
        parts = lax.all_to_all(copies, "fiber", 0, 0, axis_index_groups=far, tiled=True)
        solved = pl.pallas_call(
            solve_kernel,
            out_shape=jax.ShapeDtypeStruct((len(near[0]), PARAMS, LANES), f32),
            compiler_params=params(8),
            name="solve",
        )(parts, jnp.asarray(rebuild_rows(), f32))
        coeffs = lax.all_to_all(solved, "fiber", 0, 0, axis_index_groups=near, tiled=True)

        chi_local = pl.pallas_call(
            chi_sum_kernel,
            in_specs=[VMEM] * 4,
            out_specs=VMEM,
            out_shape=jax.ShapeDtypeStruct((8, exposures * fibers), f32),
            scratch_shapes=[pltpu.VMEM((exposures * fibers, LANES), f32)],
            compiler_params=params(16),
            cost_estimate=cost(FLOPS // 2, 0),
            name="chisum",
        )(feats, coeffs, flux, weight)
        halves = lax.axis_size("wave")
        chi_other = lax.ppermute(chi_local, "wave", [(h, (h + 1) % halves) for h in range(halves)])
        residual, sky_coeffs = pl.pallas_call(
            write_kernel,
            in_specs=[VMEM] * 3,
            out_specs=[HBM] * 2,
            out_shape=[
                jax.ShapeDtypeStruct(spectra.shape, f32),
                jax.ShapeDtypeStruct((PARAMS, waves), f32),
            ],
            scratch_shapes=[
                pltpu.VMEM(spectra.shape, f32),
                pltpu.VMEM((PARAMS, waves), f32),
                pltpu.SemaphoreType.DMA((pieces,)),
                pltpu.SemaphoreType.DMA,
            ],
            compiler_params=params(16),
            cost_estimate=cost(FLOPS, moved),
            name="residual",
        )(feats, coeffs, flux)
        chi_square = pl.pallas_call(
            functools.partial(chi_kernel, 1.0 / (waves * halves)),
            out_shape=jax.ShapeDtypeStruct((exposures, fibers), f32),
            compiler_params=params(4),
            name="chi",
        )(chi_local, chi_other)
        return residual, chi_square, sky_coeffs

    return body


def solution(mesh):
    near, far = groups((8, 4, 4))
    placed = (
        P(None, "fiber", "wave"),
        P(None, "fiber", "wave"),
        P(None, "fiber", "wave"),
        P(None, "fiber"),
        P("fiber"),
        P(),
        P(None, "fiber"),
    )
    return jax.shard_map(
        make_body(near, far),
        mesh=mesh,
        in_specs=placed,
        out_specs=(P(None, "fiber", "wave"), P(None, "fiber"), P(None, "wave")),
        check_vma=False,
    )
```

```python
import functools

import jax
import jax.numpy as jnp
from jax import lax
from jax.experimental import pallas as pl
from jax.experimental.pallas import tpu as pltpu
from jax.sharding import PartitionSpec as P

PARAMS = 16
BAD_BITS = 31
PRIOR = 1.0
MOMENTS = 7
BASIS = 4
RIGHT_ROW = 56
PACKED = 72
LANES = 128
PAIR = 1
PIECE = 512
WRITE = 1024
EARLY = 2048
GRAIN = 2048
FLOPS = 4_000_000_000


def legendre_series(coord, total):
    series = [jnp.ones_like(coord), coord]
    for order in range(1, total - 1):
        series.append(((2 * order + 1) * coord * series[order] - order * series[order - 1]) / (order + 1))
    return series


def monomial_table(total):
    coeffs = [[0.0] * total for _ in range(total)]
    coeffs[0][0] = 1.0
    coeffs[1][1] = 1.0
    for order in range(1, total - 1):
        for power in range(total):
            raised = coeffs[order][power - 1] if power >= 1 else 0.0
            coeffs[order + 1][power] = ((2 * order + 1) * raised - order * coeffs[order - 1][power]) / (order + 1)
    return coeffs


def product_series(higher, first, second):
    product = [0.0] * MOMENTS
    for left in range(MOMENTS):
        for right in range(MOMENTS - left):
            product[left + right] += higher[first][left] * higher[second][right]
    series = [0.0] * MOMENTS
    for order in reversed(range(MOMENTS)):
        now = product[order] / higher[order][order]
        series[order] = now
        for power in range(MOMENTS):
            product[power] -= now * higher[order][power]
    return series


def rebuild_rows():
    higher = monomial_table(MOMENTS)
    pair = [[product_series(higher, a, b) for b in range(BASIS)] for a in range(BASIS)]
    rows = []
    for i in range(BASIS):
        for j in range(BASIS):
            for k in range(BASIS):
                for l in range(BASIS):
                    row = [0.0] * LANES
                    for a in range(MOMENTS):
                        for b in range(MOMENTS):
                            row[a * MOMENTS + b] = pair[i][k][a] * pair[j][l][b]
                    rows.append(row)
    return rows


def split3(value):
    high = value.astype(jnp.bfloat16)
    rest = value - high.astype(jnp.float32)
    middle = rest.astype(jnp.bfloat16)
    low = (rest - middle.astype(jnp.float32)).astype(jnp.bfloat16)
    return high, middle, low


def dot6(left, right):
    l1, l2, l3 = split3(left)
    r1, r2, r3 = split3(right)
    total = None
    for a, b in ((l1, r3), (l3, r1), (l2, r2), (l1, r2), (l2, r1), (l1, r1)):
        part = jnp.dot(a, b, preferred_element_type=jnp.float32)
        total = part if total is None else total + part
    return total


def build_features(ids_ref, pos_ref, tput_ref, sky_ref, stack_ref, feat_ref, left_ref):
    exposures, fibers = tput_ref.shape
    stack_ref[0:LANES, :] = jnp.zeros((LANES, LANES), jnp.float32)
    stack_ref[0:exposures, 0:fibers] = tput_ref[...]
    stack_ref[8:8 + exposures, 0:fibers] = sky_ref[...].astype(jnp.float32)
    stack_ref[16:17, 0:fibers] = ids_ref[...].reshape(1, fibers).astype(jnp.float32)
    turned = stack_ref[0:LANES, :].T
    lane = lax.broadcasted_iota(jnp.int32, (fibers, LANES), 1)
    ids = jnp.broadcast_to(turned[0:fibers, 16:17], (fibers, LANES)).astype(jnp.int32)
    sum_x = jnp.zeros((fibers, LANES), jnp.float32)
    sum_y = jnp.zeros((fibers, LANES), jnp.float32)
    offset = ids - lane
    for tile in range(pos_ref.shape[1] // LANES):
        hit = offset == tile * LANES
        cut = slice(tile * LANES, (tile + 1) * LANES)
        sum_x = jnp.where(hit, pos_ref[0:1, cut], sum_x)
        sum_y = jnp.where(hit, pos_ref[1:2, cut], sum_y)
    coord_x = jnp.sum(sum_x, axis=1, keepdims=True)
    coord_y = jnp.sum(sum_y, axis=1, keepdims=True)
    series_x = legendre_series(jnp.broadcast_to(coord_x, (fibers, LANES)), MOMENTS)
    series_y = legendre_series(jnp.broadcast_to(coord_y, (fibers, LANES)), MOMENTS)
    is_right = lane >= RIGHT_ROW
    index_x = jnp.where(is_right, (lane - RIGHT_ROW) // BASIS, lane // MOMENTS)
    index_y = jnp.where(is_right, (lane - RIGHT_ROW) % BASIS, lane % MOMENTS)
    along_x = jnp.zeros((fibers, LANES), jnp.float32)
    along_y = jnp.zeros((fibers, LANES), jnp.float32)
    for order in range(MOMENTS):
        along_x = jnp.where(index_x == order, series_x[order], along_x)
        along_y = jnp.where(index_y == order, series_y[order], along_y)
    product = along_x * along_y
    moment_part = jnp.where(lane < MOMENTS * MOMENTS, product, 0.0)
    right_part = jnp.where(is_right & (lane < RIGHT_ROW + PARAMS), product, 0.0)
    feat_ref[0:fibers, :] = right_part
    feat_ref[fibers:2 * fibers, :] = turned[0:fibers, :]
    both = jnp.concatenate([moment_part, right_part], axis=0)
    high, middle, low = (part.astype(jnp.float32) for part in split3(both))
    rows = 2 * fibers
    for place, part in enumerate((high, middle, low, high, middle, high)):
        stack_ref[place * rows:(place + 1) * rows, :] = part
    stack_ref[6 * rows:, :] = jnp.zeros((stack_ref.shape[0] - 6 * rows, LANES), jnp.float32)
    for tile in range(stack_ref.shape[0] // LANES):
        cut = slice(tile * LANES, (tile + 1) * LANES)
        left_ref[:, cut] = stack_ref[cut, :].T[0:left_ref.shape[0], :].astype(jnp.bfloat16)


def piece_copies(flux_hbm, ivar_hbm, bits_hbm, flux_ref, ivar_ref, bits_ref, sems):
    copies = []
    for piece in range(flux_ref.shape[2] // GRAIN):
        cut = pl.ds(piece * GRAIN, GRAIN)
        copies.append([
            pltpu.make_async_copy(source.at[:, :, cut], target.at[:, :, cut], sems.at[piece, which])
            for which, (source, target) in enumerate(((flux_hbm, flux_ref), (ivar_hbm, ivar_ref), (bits_hbm, bits_ref)))
        ])
    return copies


def sum_pieces(copies, feat_ref, left_ref, flux_ref, ivar_ref, bits_ref, out_ref, weight_ref):
    exposures, fibers, _ = flux_ref.shape
    columns = feat_ref[fibers:2 * fibers, :]
    for piece in range(flux_ref.shape[2] // PIECE):
        if piece * PIECE % GRAIN == 0:
            for copy in copies[piece * PIECE // GRAIN]:
                copy.wait()
        here = slice(piece * PIECE, (piece + 1) * PIECE)
        moment_rows = None
        right_rows = None
        for e in range(exposures):
            through = columns[:, e:e + 1]
            sky = columns[:, 8 + e:9 + e]
            weight = jnp.where((bits_ref[e, :, here] & BAD_BITS) == 0, ivar_ref[e, :, here], 0.0)
            weight_ref[e, :, here] = weight
            first = weight * (through * sky)
            a = first * through
            b = first * flux_ref[e, :, here]
            moment_rows = a if e == 0 else moment_rows + a
            right_rows = b if e == 0 else right_rows + b
        high, middle, low = split3(jnp.concatenate([moment_rows, right_rows], axis=0))
        right = jnp.concatenate([high, high, high, middle, middle, low], axis=0)
        sums = jnp.dot(left_ref[:, 0:right.shape[0]], right, preferred_element_type=jnp.float32)
        for k in range(PIECE // LANES):
            out_ref[piece * (PIECE // LANES) + k] = sums[0:PACKED, k * LANES:(k + 1) * LANES]


def moments_kernel(ids_hbm, pos_hbm, tput_hbm, sky_hbm, flux_hbm, ivar_hbm, bits_hbm, out_ref, feat_ref, flux_ref, weight_ref,
                   ids_ref, pos_ref, tput_ref, sky_ref, ivar_ref, bits_ref, left_ref, stack_ref, small_sems, sems):
    small = [
        pltpu.make_async_copy(source, target, small_sems.at[place])
        for place, (source, target) in enumerate(((ids_hbm, ids_ref), (pos_hbm, pos_ref), (tput_hbm, tput_ref), (sky_hbm, sky_ref)))
    ]
    for copy in small:
        copy.start()
    copies = piece_copies(flux_hbm, ivar_hbm, bits_hbm, flux_ref, ivar_ref, bits_ref, sems)
    for place, trio in enumerate(copies):
        for which, copy in enumerate(trio):
            copy.start(priority=(place + which) % 2)
    for copy in small:
        copy.wait()
    build_features(ids_ref, pos_ref, tput_ref, sky_ref, stack_ref, feat_ref, left_ref)
    sum_pieces(copies, feat_ref, left_ref, flux_ref, ivar_ref, bits_ref, out_ref, weight_ref)


def add_kernel(in_ref, out_ref):
    total = in_ref[0]
    for source in range(1, in_ref.shape[0]):
        total = total + in_ref[source]
    for target in range(out_ref.shape[0]):
        out_ref[target] = total


def solve_one(total, table):
    moments = jnp.concatenate([total[0:RIGHT_ROW], jnp.zeros((LANES - RIGHT_ROW, LANES), jnp.float32)], axis=0)
    normal = dot6(table, moments)
    sub = lax.broadcasted_iota(jnp.int32, (PARAMS, LANES), 0)
    columns = []
    for k in range(PARAMS):
        column = normal[k * PARAMS:(k + 1) * PARAMS]
        columns.append(jnp.where(sub == k, column + PRIOR, column))
    right = total[RIGHT_ROW:RIGHT_ROW + PARAMS]
    scale = jnp.zeros((PARAMS, LANES), jnp.float32)
    for j in range(PARAMS):
        inverse = 1.0 / columns[j][j:j + 1]
        scale = jnp.where(sub == j, inverse, scale)
        factor = jnp.where(sub == j, 0.0, columns[j] * inverse)
        for l in range(j + 1, PARAMS):
            columns[l] = columns[l] - factor * columns[l][j:j + 1]
        right = right - factor * right[j:j + 1]
    return right * scale


def solve_kernel(in_ref, table_ref, out_ref):
    total = in_ref[0]
    for source in range(1, in_ref.shape[0]):
        total = total + in_ref[source]
    table = table_ref[...]
    stretches = in_ref.shape[1] // PACKED
    solved = jnp.concatenate([solve_one(total[t * PACKED:(t + 1) * PACKED], table) for t in range(stretches)], axis=0)
    for target in range(out_ref.shape[0]):
        out_ref[target] = solved


def joined(coeff_ref, first, count):
    return jnp.concatenate([coeff_ref[first + k] for k in range(count)], axis=1)


def residual_kernel(feat_ref, coeff_ref, flux_ref, weight_ref, chi_ref, late_ref, res_hbm, all_hbm, sum_ref, early_ref, all_ref, sems, all_sem):
    exposures, fibers, waves = flux_ref.shape
    chunks = waves // LANES
    early = early_ref.shape[2]
    all_ref[...] = joined(coeff_ref, 0, chunks)
    copies = [pltpu.make_async_copy(all_ref, all_hbm, all_sem)]
    copies[0].start(priority=1)
    basis = feat_ref[0:fibers, RIGHT_ROW:RIGHT_ROW + PARAMS]
    sums = [None] * exposures
    for piece in range(waves // PIECE):
        here = slice(piece * PIECE, (piece + 1) * PIECE)
        model = dot6(basis, joined(coeff_ref, piece * (PIECE // LANES), PIECE // LANES))
        for e in range(exposures):
            residual = flux_ref[e, :, here] - feat_ref[fibers:2 * fibers, e:e + 1] * model
            if piece * PIECE < early:
                early_ref[e, :, here] = residual
            else:
                late_ref[e, :, piece * PIECE - early:(piece + 1) * PIECE - early] = residual
            chi = weight_ref[e, :, here] * residual * residual
            for k in range(PIECE // LANES):
                part = chi[:, k * LANES:(k + 1) * LANES]
                sums[e] = part if sums[e] is None else sums[e] + part
        done = (piece + 1) * PIECE
        if done <= early and done % WRITE == 0:
            cut = pl.ds(done - WRITE, WRITE)
            copies.append(pltpu.make_async_copy(early_ref.at[:, :, cut], res_hbm.at[:, :, cut], sems.at[done // WRITE - 1]))
            copies[-1].start(priority=done // WRITE % 2)
    for e in range(exposures):
        sum_ref[e * fibers:(e + 1) * fibers, :] = sums[e]
    ones = jnp.ones((8, LANES), jnp.float32)
    chi_ref[...] = lax.dot_general(ones, sum_ref[...], (((1,), (1,)), ((), ())), precision=lax.Precision.HIGHEST, preferred_element_type=jnp.float32)
    for copy in copies:
        copy.wait()


def late_kernel(late_ref, _, res_hbm, sems):
    width = late_ref.shape[2]
    begin = res_hbm.shape[2] - width
    copies = [
        pltpu.make_async_copy(late_ref.at[e], res_hbm.at[e, :, pl.ds(begin, width)], sems.at[e])
        for e in range(late_ref.shape[0])
    ]
    for e, copy in enumerate(copies):
        copy.start(priority=e % 2)
    for copy in copies:
        copy.wait()


def chi_kernel(scale, mine_ref, other_ref, out_ref):
    exposures, fibers = out_ref.shape
    total = (mine_ref[...] + other_ref[...]) * scale
    for e in range(exposures):
        out_ref[e:e + 1, :] = total[0:1, e * fibers:(e + 1) * fibers]


def cost(flops, moved):
    return pl.CostEstimate(flops=flops, bytes_accessed=moved, transcendentals=0)


def params(limit_mib, dims=0):
    semantics = {"dimension_semantics": ("arbitrary",) * dims} if dims else {}
    return pltpu.CompilerParams(vmem_limit_bytes=limit_mib * 1024 * 1024, **semantics)


def groups(sizes):
    nz, ny, nx = sizes

    def place(z, y, x):
        return (z * ny + y) * nx + x

    pair = PAIR
    near = [[place(q * pair + h, y, x) for h in range(pair) for y in range(ny) for x in range(nx)] for q in range(nz // pair)]
    far = [[place(q * pair + h, y, x) for q in range(nz // pair)] for h in range(pair) for y in range(ny) for x in range(nx)]
    return near, far


VMEM = pl.BlockSpec(memory_space=pltpu.VMEM)
HBM = pl.BlockSpec(memory_space=pltpu.HBM)


def make_body(near, far):
    def body(spectra, inverse_var, mask_bits, sky_flags, fiber_ids, positions, throughput):
        exposures, fibers, waves = spectra.shape
        f32 = jnp.float32
        stacked = -(-12 * fibers // LANES) * LANES
        moved = 4 * exposures * fibers * waves

        held = [
            pltpu.with_memory_space_constraint(value, pltpu.HBM)
            for value in (fiber_ids, positions, throughput, sky_flags, spectra, inverse_var, mask_bits)
        ]
        packed, feats, flux, weight = pl.pallas_call(
            moments_kernel,
            in_specs=[HBM] * 7,
            out_specs=[VMEM] * 4,
            out_shape=[
                jax.ShapeDtypeStruct((waves // LANES, PACKED, LANES), f32),
                jax.ShapeDtypeStruct((2 * fibers, LANES), f32),
                jax.ShapeDtypeStruct(spectra.shape, f32),
                jax.ShapeDtypeStruct(spectra.shape, f32),
            ],
            scratch_shapes=[
                pltpu.VMEM(fiber_ids.shape, jnp.int32),
                pltpu.VMEM(positions.shape, f32),
                pltpu.VMEM((exposures, fibers), f32),
                pltpu.VMEM((exposures, fibers), jnp.int32),
                pltpu.VMEM(spectra.shape, f32),
                pltpu.VMEM(spectra.shape, jnp.int32),
                pltpu.VMEM((80, stacked), jnp.bfloat16),
                pltpu.VMEM((stacked, LANES), f32),
                pltpu.SemaphoreType.DMA((4,)),
                pltpu.SemaphoreType.DMA((waves // GRAIN, 3)),
            ],
            compiler_params=params(20),
            cost_estimate=cost(FLOPS, 3 * moved),
            name="moments",
        )(*held)

        members = len(near[0])
        rows = waves // LANES // members * PACKED
        packed = packed.reshape(members, rows, LANES)
        arrived = lax.all_to_all(packed, "fiber", 0, 0, axis_index_groups=near, tiled=True)
        copies = pl.pallas_call(
            add_kernel,
            out_shape=jax.ShapeDtypeStruct((len(far[0]), rows, LANES), f32),
            compiler_params=params(8),
            name="add",
        )(arrived)
        parts = lax.all_to_all(copies, "fiber", 0, 0, axis_index_groups=far, tiled=True)
        solved = pl.pallas_call(
            solve_kernel,
            out_shape=jax.ShapeDtypeStruct((members, rows // PACKED * PARAMS, LANES), f32),
            compiler_params=params(8),
            name="solve",
        )(parts, jnp.asarray(rebuild_rows(), f32))
        coeffs = lax.all_to_all(solved, "fiber", 0, 0, axis_index_groups=near, tiled=True)
        coeffs = coeffs.reshape(waves // LANES, PARAMS, LANES)

        chi_local, late, residual, sky_coeffs = pl.pallas_call(
            residual_kernel,
            in_specs=[VMEM] * 4,
            out_specs=[VMEM, VMEM, HBM, HBM],
            out_shape=[
                jax.ShapeDtypeStruct((8, exposures * fibers), f32),
                jax.ShapeDtypeStruct((exposures, fibers, waves - EARLY), f32),
                jax.ShapeDtypeStruct(spectra.shape, f32),
                jax.ShapeDtypeStruct((PARAMS, waves), f32),
            ],
            scratch_shapes=[
                pltpu.VMEM((exposures * fibers, LANES), f32),
                pltpu.VMEM((exposures, fibers, EARLY), f32),
                pltpu.VMEM((PARAMS, waves), f32),
                pltpu.SemaphoreType.DMA((EARLY // WRITE,)),
                pltpu.SemaphoreType.DMA,
            ],
            compiler_params=params(16),
            cost_estimate=cost(FLOPS, moved),
            name="residual",
        )(feats, coeffs, flux, weight)
        halves = lax.axis_size("wave")
        chi_other = lax.ppermute(chi_local, "wave", [(h, (h + 1) % halves) for h in range(halves)])
        residual = pl.pallas_call(
            late_kernel,
            in_specs=[VMEM, HBM],
            out_specs=HBM,
            out_shape=jax.ShapeDtypeStruct(spectra.shape, f32),
            input_output_aliases={1: 0},
            scratch_shapes=[pltpu.SemaphoreType.DMA((exposures,))],
            compiler_params=params(4),
            cost_estimate=cost(FLOPS, moved),
            name="late",
        )(late, residual)
        chi_square = pl.pallas_call(
            functools.partial(chi_kernel, 1.0 / (waves * halves)),
            out_shape=jax.ShapeDtypeStruct((exposures, fibers), f32),
            compiler_params=params(4),
            name="chi",
        )(chi_local, chi_other)
        return residual, chi_square, sky_coeffs

    return body


def solution(mesh):
    near, far = groups((8, 4, 4))
    placed = (
        P(None, "fiber", "wave"),
        P(None, "fiber", "wave"),
        P(None, "fiber", "wave"),
        P(None, "fiber"),
        P("fiber"),
        P(),
        P(None, "fiber"),
    )
    return jax.shard_map(
        make_body(near, far),
        mesh=mesh,
        in_specs=placed,
        out_specs=(P(None, "fiber", "wave"), P(None, "fiber"), P(None, "wave")),
        check_vma=False,
    )
```

```python
import functools

import jax
import jax.numpy as jnp
from jax import lax
from jax.experimental import pallas as pl
from jax.experimental.pallas import tpu as pltpu
from jax.sharding import PartitionSpec as P

PARAMS = 16
BAD_BITS = 31
PRIOR = 1.0
MOMENTS = 7
BASIS = 4
RIGHT_ROW = 49
PACKED = 65
ROWS = 72
LANES = 128
PIECE = 512
WRITE = 1024
EARLY = 2048
GRAIN = 2048
FLOPS = 4_000_000_000


def legendre_series(coord, total):
    series = [jnp.ones_like(coord), coord]
    for order in range(1, total - 1):
        series.append(((2 * order + 1) * coord * series[order] - order * series[order - 1]) / (order + 1))
    return series


def monomial_table(total):
    coeffs = [[0.0] * total for _ in range(total)]
    coeffs[0][0] = 1.0
    coeffs[1][1] = 1.0
    for order in range(1, total - 1):
        for power in range(total):
            raised = coeffs[order][power - 1] if power >= 1 else 0.0
            coeffs[order + 1][power] = ((2 * order + 1) * raised - order * coeffs[order - 1][power]) / (order + 1)
    return coeffs


def product_series(higher, first, second):
    product = [0.0] * MOMENTS
    for left in range(MOMENTS):
        for right in range(MOMENTS - left):
            product[left + right] += higher[first][left] * higher[second][right]
    series = [0.0] * MOMENTS
    for order in reversed(range(MOMENTS)):
        now = product[order] / higher[order][order]
        series[order] = now
        for power in range(MOMENTS):
            product[power] -= now * higher[order][power]
    return series


def rebuild_rows():
    higher = monomial_table(MOMENTS)
    pair = [[product_series(higher, a, b) for b in range(BASIS)] for a in range(BASIS)]
    rows = []
    for i in range(BASIS):
        for j in range(BASIS):
            for k in range(BASIS):
                for l in range(BASIS):
                    row = [0.0] * LANES
                    for a in range(MOMENTS):
                        for b in range(MOMENTS):
                            row[a * MOMENTS + b] = pair[i][k][a] * pair[j][l][b]
                    rows.append(row)
    return rows


def split3(value):
    high = value.astype(jnp.bfloat16)
    rest = value - high.astype(jnp.float32)
    middle = rest.astype(jnp.bfloat16)
    low = (rest - middle.astype(jnp.float32)).astype(jnp.bfloat16)
    return high, middle, low


def dot6(left, right):
    l1, l2, l3 = split3(left)
    r1, r2, r3 = split3(right)
    total = None
    for a, b in ((l1, r3), (l3, r1), (l2, r2), (l1, r2), (l2, r1), (l1, r1)):
        part = jnp.dot(a, b, preferred_element_type=jnp.float32)
        total = part if total is None else total + part
    return total


def build_features(ids_ref, pos_ref, tput_ref, sky_ref, stack_ref, feat_ref, left_ref):
    exposures, fibers = tput_ref.shape
    stack_ref[0:LANES, :] = jnp.zeros((LANES, LANES), jnp.float32)
    stack_ref[0:exposures, 0:fibers] = tput_ref[...]
    stack_ref[8:8 + exposures, 0:fibers] = sky_ref[...].astype(jnp.float32)
    stack_ref[16:17, 0:fibers] = ids_ref[...].reshape(1, fibers).astype(jnp.float32)
    turned = stack_ref[0:LANES, :].T
    lane = lax.broadcasted_iota(jnp.int32, (fibers, LANES), 1)
    ids = jnp.broadcast_to(turned[0:fibers, 16:17], (fibers, LANES)).astype(jnp.int32)
    sum_x = jnp.zeros((fibers, LANES), jnp.float32)
    sum_y = jnp.zeros((fibers, LANES), jnp.float32)
    offset = ids - lane
    for tile in range(pos_ref.shape[1] // LANES):
        hit = offset == tile * LANES
        cut = slice(tile * LANES, (tile + 1) * LANES)
        sum_x = jnp.where(hit, pos_ref[0:1, cut], sum_x)
        sum_y = jnp.where(hit, pos_ref[1:2, cut], sum_y)
    coord_x = jnp.sum(sum_x, axis=1, keepdims=True)
    coord_y = jnp.sum(sum_y, axis=1, keepdims=True)
    series_x = legendre_series(jnp.broadcast_to(coord_x, (fibers, LANES)), MOMENTS)
    series_y = legendre_series(jnp.broadcast_to(coord_y, (fibers, LANES)), MOMENTS)
    is_right = lane >= RIGHT_ROW
    index_x = jnp.where(is_right, (lane - RIGHT_ROW) // BASIS, lane // MOMENTS)
    index_y = jnp.where(is_right, (lane - RIGHT_ROW) % BASIS, lane % MOMENTS)
    along_x = jnp.zeros((fibers, LANES), jnp.float32)
    along_y = jnp.zeros((fibers, LANES), jnp.float32)
    for order in range(MOMENTS):
        along_x = jnp.where(index_x == order, series_x[order], along_x)
        along_y = jnp.where(index_y == order, series_y[order], along_y)
    product = along_x * along_y
    moment_part = jnp.where(lane < MOMENTS * MOMENTS, product, 0.0)
    right_part = jnp.where(is_right & (lane < RIGHT_ROW + PARAMS), product, 0.0)
    feat_ref[0:fibers, :] = right_part
    feat_ref[fibers:2 * fibers, :] = turned[0:fibers, :]
    both = jnp.concatenate([moment_part, right_part], axis=0)
    high, middle, low = (part.astype(jnp.float32) for part in split3(both))
    rows = 2 * fibers
    for place, part in enumerate((high, middle, low, high, middle, high)):
        stack_ref[place * rows:(place + 1) * rows, :] = part
    stack_ref[6 * rows:, :] = jnp.zeros((stack_ref.shape[0] - 6 * rows, LANES), jnp.float32)
    for tile in range(stack_ref.shape[0] // LANES):
        cut = slice(tile * LANES, (tile + 1) * LANES)
        left_ref[:, cut] = stack_ref[cut, :].T[0:left_ref.shape[0], :].astype(jnp.bfloat16)


def piece_copies(flux_hbm, ivar_hbm, bits_hbm, flux_ref, ivar_ref, bits_ref, sems):
    copies = []
    for piece in range(flux_ref.shape[2] // GRAIN):
        cut = pl.ds(piece * GRAIN, GRAIN)
        copies.append([
            pltpu.make_async_copy(source.at[:, :, cut], target.at[:, :, cut], sems.at[piece, which])
            for which, (source, target) in enumerate(((flux_hbm, flux_ref), (ivar_hbm, ivar_ref), (bits_hbm, bits_ref)))
        ])
    return copies


def sum_pieces(copies, feat_ref, left_ref, flux_ref, ivar_ref, bits_ref, out_ref, weight_ref):
    exposures, fibers, _ = flux_ref.shape
    columns = feat_ref[fibers:2 * fibers, :]
    for piece in range(flux_ref.shape[2] // PIECE):
        if piece * PIECE % GRAIN == 0:
            for copy in copies[piece * PIECE // GRAIN]:
                copy.wait()
        here = slice(piece * PIECE, (piece + 1) * PIECE)
        moment_rows = None
        right_rows = None
        for e in range(exposures):
            through = columns[:, e:e + 1]
            sky = columns[:, 8 + e:9 + e]
            weight = jnp.where((bits_ref[e, :, here] & BAD_BITS) == 0, ivar_ref[e, :, here], 0.0)
            weight_ref[e, :, here] = weight
            first = weight * (through * sky)
            a = first * through
            b = first * flux_ref[e, :, here]
            moment_rows = a if e == 0 else moment_rows + a
            right_rows = b if e == 0 else right_rows + b
        high, middle, low = split3(jnp.concatenate([moment_rows, right_rows], axis=0))
        right = jnp.concatenate([high, high, high, middle, middle, low], axis=0)
        sums = jnp.dot(left_ref[:, 0:right.shape[0]], right, preferred_element_type=jnp.float32)
        for k in range(PIECE // LANES):
            chunk = piece * (PIECE // LANES) + k
            out_ref[chunk * PACKED:(chunk + 1) * PACKED, :] = sums[0:PACKED, k * LANES:(k + 1) * LANES]


def moments_kernel(ids_hbm, pos_hbm, tput_hbm, sky_hbm, flux_hbm, ivar_hbm, bits_hbm, out_ref, feat_ref, flux_ref, weight_ref,
                   ids_ref, pos_ref, tput_ref, sky_ref, ivar_ref, bits_ref, left_ref, stack_ref, small_sems, sems):
    small = [
        pltpu.make_async_copy(source, target, small_sems.at[place])
        for place, (source, target) in enumerate(((ids_hbm, ids_ref), (pos_hbm, pos_ref), (tput_hbm, tput_ref), (sky_hbm, sky_ref)))
    ]
    for copy in small:
        copy.start()
    copies = piece_copies(flux_hbm, ivar_hbm, bits_hbm, flux_ref, ivar_ref, bits_ref, sems)
    for place, trio in enumerate(copies):
        for which, copy in enumerate(trio):
            copy.start(priority=(place + which) % 2)
    for copy in small:
        copy.wait()
    build_features(ids_ref, pos_ref, tput_ref, sky_ref, stack_ref, feat_ref, left_ref)
    sum_pieces(copies, feat_ref, left_ref, flux_ref, ivar_ref, bits_ref, out_ref, weight_ref)


def add_kernel(in_ref, out_ref):
    total = in_ref[0:PACKED, :]
    for source in range(1, in_ref.shape[0] // PACKED):
        total = total + in_ref[source * PACKED:(source + 1) * PACKED, :]
    total = jnp.concatenate([total, jnp.zeros((ROWS - PACKED, LANES), jnp.float32)], axis=0)
    for target in range(out_ref.shape[0]):
        out_ref[target] = total


def solve_kernel(in_ref, table_ref, out_ref):
    total = in_ref[0]
    for source in range(1, in_ref.shape[0]):
        total = total + in_ref[source]
    normal = dot6(table_ref[...], jnp.concatenate([total, jnp.zeros((LANES - ROWS, LANES), jnp.float32)], axis=0))
    sub = lax.broadcasted_iota(jnp.int32, (PARAMS, LANES), 0)
    columns = []
    for k in range(PARAMS):
        column = normal[k * PARAMS:(k + 1) * PARAMS]
        columns.append(jnp.where(sub == k, column + PRIOR, column))
    right = total[RIGHT_ROW:RIGHT_ROW + PARAMS]
    scale = jnp.zeros((PARAMS, LANES), jnp.float32)
    for j in range(PARAMS):
        inverse = 1.0 / columns[j][j:j + 1]
        scale = jnp.where(sub == j, inverse, scale)
        factor = jnp.where(sub == j, 0.0, columns[j] * inverse)
        for l in range(j + 1, PARAMS):
            columns[l] = columns[l] - factor * columns[l][j:j + 1]
        right = right - factor * right[j:j + 1]
    solved = right * scale
    for target in range(out_ref.shape[0]):
        out_ref[target] = solved


def joined(coeff_ref, first, count):
    return jnp.concatenate([coeff_ref[first + k] for k in range(count)], axis=1)


def residual_kernel(feat_ref, coeff_ref, flux_ref, weight_ref, chi_ref, late_ref, res_hbm, all_hbm, sum_ref, early_ref, all_ref, sems, all_sem):
    exposures, fibers, waves = flux_ref.shape
    chunks = waves // LANES
    early = early_ref.shape[2]
    all_ref[...] = joined(coeff_ref, 0, chunks)
    copies = [pltpu.make_async_copy(all_ref, all_hbm, all_sem)]
    copies[0].start(priority=1)
    basis = feat_ref[0:fibers, RIGHT_ROW:RIGHT_ROW + PARAMS]
    sums = [None] * exposures
    for piece in range(waves // PIECE):
        here = slice(piece * PIECE, (piece + 1) * PIECE)
        model = dot6(basis, joined(coeff_ref, piece * (PIECE // LANES), PIECE // LANES))
        for e in range(exposures):
            residual = flux_ref[e, :, here] - feat_ref[fibers:2 * fibers, e:e + 1] * model
            if piece * PIECE < early:
                early_ref[e, :, here] = residual
            else:
                late_ref[e, :, piece * PIECE - early:(piece + 1) * PIECE - early] = residual
            chi = weight_ref[e, :, here] * residual * residual
            for k in range(PIECE // LANES):
                part = chi[:, k * LANES:(k + 1) * LANES]
                sums[e] = part if sums[e] is None else sums[e] + part
        done = (piece + 1) * PIECE
        if done <= early and done % WRITE == 0:
            cut = pl.ds(done - WRITE, WRITE)
            copies.append(pltpu.make_async_copy(early_ref.at[:, :, cut], res_hbm.at[:, :, cut], sems.at[done // WRITE - 1]))
            copies[-1].start(priority=done // WRITE % 2)
    for e in range(exposures):
        sum_ref[e * fibers:(e + 1) * fibers, :] = sums[e]
    ones = jnp.ones((8, LANES), jnp.float32)
    chi_ref[...] = lax.dot_general(ones, sum_ref[...], (((1,), (1,)), ((), ())), precision=lax.Precision.HIGHEST, preferred_element_type=jnp.float32)
    for copy in copies:
        copy.wait()


def late_kernel(late_ref, _, res_hbm, sems):
    width = late_ref.shape[2]
    begin = res_hbm.shape[2] - width
    copies = [
        pltpu.make_async_copy(late_ref.at[e], res_hbm.at[e, :, pl.ds(begin, width)], sems.at[e])
        for e in range(late_ref.shape[0])
    ]
    for e, copy in enumerate(copies):
        copy.start(priority=e % 2)
    for copy in copies:
        copy.wait()


def chi_kernel(scale, mine_ref, other_ref, out_ref):
    exposures, fibers = out_ref.shape
    total = (mine_ref[...] + other_ref[...]) * scale
    for e in range(exposures):
        out_ref[e:e + 1, :] = total[0:1, e * fibers:(e + 1) * fibers]


def cost(flops, moved):
    return pl.CostEstimate(flops=flops, bytes_accessed=moved, transcendentals=0)


def params(limit_mib, dims=0):
    semantics = {"dimension_semantics": ("arbitrary",) * dims} if dims else {}
    return pltpu.CompilerParams(vmem_limit_bytes=limit_mib * 1024 * 1024, **semantics)


def groups(sizes):
    nz, ny, nx = sizes

    def place(z, y, x):
        return (z * ny + y) * nx + x

    pair = 2
    near = [[place(q * pair + h, y, x) for h in range(pair) for y in range(ny) for x in range(nx)] for q in range(nz // pair)]
    far = [[place(q * pair + h, y, x) for q in range(nz // pair)] for h in range(pair) for y in range(ny) for x in range(nx)]
    return near, far


VMEM = pl.BlockSpec(memory_space=pltpu.VMEM)
HBM = pl.BlockSpec(memory_space=pltpu.HBM)


def make_body(near, far):
    def body(spectra, inverse_var, mask_bits, sky_flags, fiber_ids, positions, throughput):
        exposures, fibers, waves = spectra.shape
        f32 = jnp.float32
        stacked = -(-12 * fibers // LANES) * LANES
        moved = 4 * exposures * fibers * waves

        held = [
            pltpu.with_memory_space_constraint(value, pltpu.HBM)
            for value in (fiber_ids, positions, throughput, sky_flags, spectra, inverse_var, mask_bits)
        ]
        packed, feats, flux, weight = pl.pallas_call(
            moments_kernel,
            in_specs=[HBM] * 7,
            out_specs=[VMEM] * 4,
            out_shape=[
                jax.ShapeDtypeStruct((waves // LANES * PACKED, LANES), f32),
                jax.ShapeDtypeStruct((2 * fibers, LANES), f32),
                jax.ShapeDtypeStruct(spectra.shape, f32),
                jax.ShapeDtypeStruct(spectra.shape, f32),
            ],
            scratch_shapes=[
                pltpu.VMEM(fiber_ids.shape, jnp.int32),
                pltpu.VMEM(positions.shape, f32),
                pltpu.VMEM((exposures, fibers), f32),
                pltpu.VMEM((exposures, fibers), jnp.int32),
                pltpu.VMEM(spectra.shape, f32),
                pltpu.VMEM(spectra.shape, jnp.int32),
                pltpu.VMEM((80, stacked), jnp.bfloat16),
                pltpu.VMEM((stacked, LANES), f32),
                pltpu.SemaphoreType.DMA((4,)),
                pltpu.SemaphoreType.DMA((waves // GRAIN, 3)),
            ],
            compiler_params=params(20),
            cost_estimate=cost(FLOPS, 3 * moved),
            name="moments",
        )(*held)

        members = len(near[0])
        packed = packed.reshape(members, PACKED, 1, LANES)
        arrived = lax.all_to_all(packed, "fiber", 0, 0, axis_index_groups=near, tiled=True)
        copies = pl.pallas_call(
            add_kernel,
            out_shape=jax.ShapeDtypeStruct((len(far[0]), ROWS, LANES), f32),
            compiler_params=params(8),
            name="add",
        )(arrived.reshape(members * PACKED, LANES))
        parts = lax.all_to_all(copies, "fiber", 0, 0, axis_index_groups=far, tiled=True)
        solved = pl.pallas_call(
            solve_kernel,
            out_shape=jax.ShapeDtypeStruct((members, PARAMS, LANES), f32),
            compiler_params=params(8),
            name="solve",
        )(parts, jnp.asarray(rebuild_rows(), f32))
        coeffs = lax.all_to_all(solved, "fiber", 0, 0, axis_index_groups=near, tiled=True)

        chi_local, late, residual, sky_coeffs = pl.pallas_call(
            residual_kernel,
            in_specs=[VMEM] * 4,
            out_specs=[VMEM, VMEM, HBM, HBM],
            out_shape=[
                jax.ShapeDtypeStruct((8, exposures * fibers), f32),
                jax.ShapeDtypeStruct((exposures, fibers, waves - EARLY), f32),
                jax.ShapeDtypeStruct(spectra.shape, f32),
                jax.ShapeDtypeStruct((PARAMS, waves), f32),
            ],
            scratch_shapes=[
                pltpu.VMEM((exposures * fibers, LANES), f32),
                pltpu.VMEM((exposures, fibers, EARLY), f32),
                pltpu.VMEM((PARAMS, waves), f32),
                pltpu.SemaphoreType.DMA((EARLY // WRITE,)),
                pltpu.SemaphoreType.DMA,
            ],
            compiler_params=params(16),
            cost_estimate=cost(FLOPS, moved),
            name="residual",
        )(feats, coeffs, flux, weight)
        halves = lax.axis_size("wave")
        chi_other = lax.ppermute(chi_local, "wave", [(h, (h + 1) % halves) for h in range(halves)])
        residual = pl.pallas_call(
            late_kernel,
            in_specs=[VMEM, HBM],
            out_specs=HBM,
            out_shape=jax.ShapeDtypeStruct(spectra.shape, f32),
            input_output_aliases={1: 0},
            scratch_shapes=[pltpu.SemaphoreType.DMA((exposures,))],
            compiler_params=params(4),
            cost_estimate=cost(FLOPS, moved),
            name="late",
        )(late, residual)
        chi_square = pl.pallas_call(
            functools.partial(chi_kernel, 1.0 / (waves * halves)),
            out_shape=jax.ShapeDtypeStruct((exposures, fibers), f32),
            compiler_params=params(4),
            name="chi",
        )(chi_local, chi_other)
        return residual, chi_square, sky_coeffs

    return body


def solution(mesh):
    near, far = groups((8, 4, 4))
    placed = (
        P(None, "fiber", "wave"),
        P(None, "fiber", "wave"),
        P(None, "fiber", "wave"),
        P(None, "fiber"),
        P("fiber"),
        P(),
        P(None, "fiber"),
    )
    return jax.shard_map(
        make_body(near, far),
        mesh=mesh,
        in_specs=placed,
        out_specs=(P(None, "fiber", "wave"), P(None, "fiber"), P(None, "wave")),
        check_vma=False,
    )
```

```python
import functools

import jax
import jax.numpy as jnp
from jax import lax
from jax.experimental import pallas as pl
from jax.experimental.pallas import tpu as pltpu
from jax.sharding import PartitionSpec as P

PARAMS = 16
BAD_BITS = 31
PRIOR = 1.0
MOMENTS = 7
BASIS = 4
RIGHT_ROW = 49
PACKED = 65
ROWS = 72
LANES = 128
PIECE = 512
WRITE = 1024
EARLY = 3072
GRAINS = (2048, 1024, 1024)
FLOPS = 4_000_000_000


def legendre_series(coord, total):
    series = [jnp.ones_like(coord), coord]
    for order in range(1, total - 1):
        series.append(((2 * order + 1) * coord * series[order] - order * series[order - 1]) / (order + 1))
    return series


def monomial_table(total):
    coeffs = [[0.0] * total for _ in range(total)]
    coeffs[0][0] = 1.0
    coeffs[1][1] = 1.0
    for order in range(1, total - 1):
        for power in range(total):
            raised = coeffs[order][power - 1] if power >= 1 else 0.0
            coeffs[order + 1][power] = ((2 * order + 1) * raised - order * coeffs[order - 1][power]) / (order + 1)
    return coeffs


def product_series(higher, first, second):
    product = [0.0] * MOMENTS
    for left in range(MOMENTS):
        for right in range(MOMENTS - left):
            product[left + right] += higher[first][left] * higher[second][right]
    series = [0.0] * MOMENTS
    for order in reversed(range(MOMENTS)):
        now = product[order] / higher[order][order]
        series[order] = now
        for power in range(MOMENTS):
            product[power] -= now * higher[order][power]
    return series


def rebuild_rows():
    higher = monomial_table(MOMENTS)
    pair = [[product_series(higher, a, b) for b in range(BASIS)] for a in range(BASIS)]
    rows = []
    for i in range(BASIS):
        for j in range(BASIS):
            for k in range(BASIS):
                for l in range(BASIS):
                    row = [0.0] * LANES
                    for a in range(MOMENTS):
                        for b in range(MOMENTS):
                            row[a * MOMENTS + b] = pair[i][k][a] * pair[j][l][b]
                    rows.append(row)
    return rows


def split3(value):
    high = value.astype(jnp.bfloat16)
    rest = value - high.astype(jnp.float32)
    middle = rest.astype(jnp.bfloat16)
    low = (rest - middle.astype(jnp.float32)).astype(jnp.bfloat16)
    return high, middle, low


def dot6(left, right):
    l1, l2, l3 = split3(left)
    r1, r2, r3 = split3(right)
    total = None
    for a, b in ((l1, r3), (l3, r1), (l2, r2), (l1, r2), (l2, r1), (l1, r1)):
        part = jnp.dot(a, b, preferred_element_type=jnp.float32)
        total = part if total is None else total + part
    return total


def build_features(ids_ref, pos_ref, tput_ref, sky_ref, stack_ref, feat_ref, left_ref):
    exposures, fibers = tput_ref.shape
    stack_ref[0:LANES, :] = jnp.zeros((LANES, LANES), jnp.float32)
    stack_ref[0:exposures, 0:fibers] = tput_ref[...]
    stack_ref[8:8 + exposures, 0:fibers] = sky_ref[...].astype(jnp.float32)
    stack_ref[16:17, 0:fibers] = ids_ref[...].reshape(1, fibers).astype(jnp.float32)
    turned = stack_ref[0:LANES, :].T
    lane = lax.broadcasted_iota(jnp.int32, (fibers, LANES), 1)
    ids = jnp.broadcast_to(turned[0:fibers, 16:17], (fibers, LANES)).astype(jnp.int32)
    sum_x = jnp.zeros((fibers, LANES), jnp.float32)
    sum_y = jnp.zeros((fibers, LANES), jnp.float32)
    offset = ids - lane
    for tile in range(pos_ref.shape[1] // LANES):
        hit = offset == tile * LANES
        cut = slice(tile * LANES, (tile + 1) * LANES)
        sum_x = jnp.where(hit, pos_ref[0:1, cut], sum_x)
        sum_y = jnp.where(hit, pos_ref[1:2, cut], sum_y)
    coord_x = jnp.sum(sum_x, axis=1, keepdims=True)
    coord_y = jnp.sum(sum_y, axis=1, keepdims=True)
    series_x = legendre_series(jnp.broadcast_to(coord_x, (fibers, LANES)), MOMENTS)
    series_y = legendre_series(jnp.broadcast_to(coord_y, (fibers, LANES)), MOMENTS)
    is_right = lane >= RIGHT_ROW

    def products(index_x, index_y):
        along_x = jnp.zeros((fibers, LANES), jnp.float32)
        along_y = jnp.zeros((fibers, LANES), jnp.float32)
        for order in range(MOMENTS):
            along_x = jnp.where(index_x == order, series_x[order], along_x)
            along_y = jnp.where(index_y == order, series_y[order], along_y)
        return along_x * along_y

    product = products(
        jnp.where(is_right, (lane - RIGHT_ROW) // BASIS, lane // MOMENTS),
        jnp.where(is_right, (lane - RIGHT_ROW) % BASIS, lane % MOMENTS),
    )
    group = lane // PARAMS
    model_parts = [part.astype(jnp.float32) for part in split3(products(lane % PARAMS // BASIS, lane % BASIS))]
    model_left = jnp.where((group == 1) | (group == 4), model_parts[1], jnp.where(group == 2, model_parts[2], model_parts[0]))
    moment_part = jnp.where(lane < MOMENTS * MOMENTS, product, 0.0)
    right_part = jnp.where(is_right & (lane < RIGHT_ROW + PARAMS), product, 0.0)
    feat_ref[0:fibers, :] = model_left
    feat_ref[fibers:2 * fibers, :] = turned[0:fibers, :]
    both = jnp.concatenate([moment_part, right_part], axis=0)
    high, middle, low = (part.astype(jnp.float32) for part in split3(both))
    rows = 2 * fibers
    for place, part in enumerate((high, middle, low, high, middle, high)):
        stack_ref[place * rows:(place + 1) * rows, :] = part
    stack_ref[6 * rows:, :] = jnp.zeros((stack_ref.shape[0] - 6 * rows, LANES), jnp.float32)
    for tile in range(stack_ref.shape[0] // LANES):
        cut = slice(tile * LANES, (tile + 1) * LANES)
        left_ref[:, cut] = stack_ref[cut, :].T[0:left_ref.shape[0], :].astype(jnp.bfloat16)


def piece_copies(flux_hbm, ivar_hbm, bits_hbm, flux_ref, ivar_ref, bits_ref, sems):
    copies = {}
    begin = 0
    for place, width in enumerate(GRAINS):
        cut = pl.ds(begin, width)
        copies[begin] = [
            pltpu.make_async_copy(source.at[:, :, cut], target.at[:, :, cut], sems.at[place, which])
            for which, (source, target) in enumerate(((flux_hbm, flux_ref), (ivar_hbm, ivar_ref), (bits_hbm, bits_ref)))
        ]
        begin += width
    return copies


def sum_pieces(copies, feat_ref, left_ref, flux_ref, ivar_ref, bits_ref, out_ref, weight_ref):
    exposures, fibers, _ = flux_ref.shape
    columns = feat_ref[fibers:2 * fibers, :]
    for piece in range(flux_ref.shape[2] // PIECE):
        for copy in copies.get(piece * PIECE, ()):
            copy.wait()
        here = slice(piece * PIECE, (piece + 1) * PIECE)
        moment_rows = None
        right_rows = None
        for e in range(exposures):
            through = columns[:, e:e + 1]
            sky = columns[:, 8 + e:9 + e]
            weight = jnp.where((bits_ref[e, :, here] & BAD_BITS) == 0, ivar_ref[e, :, here], 0.0)
            weight_ref[e, :, here] = weight
            first = weight * (through * sky)
            a = first * through
            b = first * flux_ref[e, :, here]
            moment_rows = a if e == 0 else moment_rows + a
            right_rows = b if e == 0 else right_rows + b
        high, middle, low = split3(jnp.concatenate([moment_rows, right_rows], axis=0))
        right = jnp.concatenate([high, high, high, middle, middle, low], axis=0)
        sums = jnp.dot(left_ref[:, 0:right.shape[0]], right, preferred_element_type=jnp.float32)
        for k in range(PIECE // LANES):
            chunk = piece * (PIECE // LANES) + k
            out_ref[chunk * PACKED:(chunk + 1) * PACKED, :] = sums[0:PACKED, k * LANES:(k + 1) * LANES]


def moments_kernel(ids_hbm, pos_hbm, tput_hbm, sky_hbm, flux_hbm, ivar_hbm, bits_hbm, out_ref, feat_ref, flux_ref, weight_ref,
                   ids_ref, pos_ref, tput_ref, sky_ref, ivar_ref, bits_ref, left_ref, stack_ref, small_sems, sems):
    small = [
        pltpu.make_async_copy(source, target, small_sems.at[place])
        for place, (source, target) in enumerate(((ids_hbm, ids_ref), (pos_hbm, pos_ref), (tput_hbm, tput_ref), (sky_hbm, sky_ref)))
    ]
    for copy in small:
        copy.start()
    copies = piece_copies(flux_hbm, ivar_hbm, bits_hbm, flux_ref, ivar_ref, bits_ref, sems)
    for begin, trio in copies.items():
        for which, copy in enumerate(trio):
            copy.start(priority=(which + (begin > 0)) % 2)
    for copy in small:
        copy.wait()
    build_features(ids_ref, pos_ref, tput_ref, sky_ref, stack_ref, feat_ref, left_ref)
    sum_pieces(copies, feat_ref, left_ref, flux_ref, ivar_ref, bits_ref, out_ref, weight_ref)


def add_kernel(in_ref, out_ref):
    total = in_ref[0:PACKED, :]
    for source in range(1, in_ref.shape[0] // PACKED):
        total = total + in_ref[source * PACKED:(source + 1) * PACKED, :]
    total = jnp.concatenate([total, jnp.zeros((ROWS - PACKED, LANES), jnp.float32)], axis=0)
    for target in range(out_ref.shape[0]):
        out_ref[target] = total


def solve_kernel(in_ref, table_ref, out_ref):
    total = in_ref[0]
    for source in range(1, in_ref.shape[0]):
        total = total + in_ref[source]
    normal = dot6(table_ref[...], jnp.concatenate([total, jnp.zeros((LANES - ROWS, LANES), jnp.float32)], axis=0))
    sub = lax.broadcasted_iota(jnp.int32, (PARAMS, LANES), 0)
    columns = []
    for k in range(PARAMS):
        column = normal[k * PARAMS:(k + 1) * PARAMS]
        columns.append(jnp.where(sub == k, column + PRIOR, column))
    right = total[RIGHT_ROW:RIGHT_ROW + PARAMS]
    scale = jnp.zeros((PARAMS, LANES), jnp.float32)
    for j in range(PARAMS):
        inverse = 1.0 / columns[j][j:j + 1]
        scale = jnp.where(sub == j, inverse, scale)
        factor = jnp.where(sub == j, 0.0, columns[j] * inverse)
        for l in range(j + 1, PARAMS):
            columns[l] = columns[l] - factor * columns[l][j:j + 1]
        right = right - factor * right[j:j + 1]
    solved = right * scale
    for target in range(out_ref.shape[0]):
        out_ref[target] = solved


def joined(coeff_ref, first, count):
    return jnp.concatenate([coeff_ref[first + k] for k in range(count)], axis=1)


def residual_kernel(feat_ref, coeff_ref, flux_ref, weight_ref, chi_ref, late_ref, res_hbm, all_hbm, sum_ref, early_ref, all_ref, sems, all_sem):
    exposures, fibers, waves = flux_ref.shape
    chunks = waves // LANES
    early = early_ref.shape[2]
    all_ref[...] = joined(coeff_ref, 0, chunks)
    copies = [pltpu.make_async_copy(all_ref, all_hbm, all_sem)]
    copies[0].start(priority=1)
    basis = feat_ref[0:fibers, 0:6 * PARAMS].astype(jnp.bfloat16)
    sums = [None] * exposures
    for piece in range(waves // PIECE):
        here = slice(piece * PIECE, (piece + 1) * PIECE)
        high, middle, low = split3(joined(coeff_ref, piece * (PIECE // LANES), PIECE // LANES))
        model = jnp.dot(basis, jnp.concatenate([high, high, high, middle, middle, low], axis=0), preferred_element_type=jnp.float32)
        for e in range(exposures):
            residual = flux_ref[e, :, here] - feat_ref[fibers:2 * fibers, e:e + 1] * model
            if piece * PIECE < early:
                early_ref[e, :, here] = residual
            else:
                late_ref[e, :, piece * PIECE - early:(piece + 1) * PIECE - early] = residual
            chi = weight_ref[e, :, here] * residual * residual
            for k in range(PIECE // LANES):
                part = chi[:, k * LANES:(k + 1) * LANES]
                sums[e] = part if sums[e] is None else sums[e] + part
        done = (piece + 1) * PIECE
        if done <= early and done % WRITE == 0:
            cut = pl.ds(done - WRITE, WRITE)
            copies.append(pltpu.make_async_copy(early_ref.at[:, :, cut], res_hbm.at[:, :, cut], sems.at[done // WRITE - 1]))
            copies[-1].start(priority=done // WRITE % 2)
    for e in range(exposures):
        sum_ref[e * fibers:(e + 1) * fibers, :] = sums[e]
    ones = jnp.ones((8, LANES), jnp.float32)
    chi_ref[...] = lax.dot_general(ones, sum_ref[...], (((1,), (1,)), ((), ())), precision=lax.Precision.HIGHEST, preferred_element_type=jnp.float32)
    for copy in copies:
        copy.wait()


def late_kernel(late_ref, _, res_hbm, sems):
    width = late_ref.shape[2]
    begin = res_hbm.shape[2] - width
    copies = [
        pltpu.make_async_copy(late_ref.at[e], res_hbm.at[e, :, pl.ds(begin, width)], sems.at[e])
        for e in range(late_ref.shape[0])
    ]
    for e, copy in enumerate(copies):
        copy.start(priority=e % 2)
    for copy in copies:
        copy.wait()


def chi_kernel(scale, mine_ref, other_ref, out_ref):
    exposures, fibers = out_ref.shape
    total = (mine_ref[...] + other_ref[...]) * scale
    for e in range(exposures):
        out_ref[e:e + 1, :] = total[0:1, e * fibers:(e + 1) * fibers]


def cost(flops, moved):
    return pl.CostEstimate(flops=flops, bytes_accessed=moved, transcendentals=0)


def params(limit_mib, dims=0):
    semantics = {"dimension_semantics": ("arbitrary",) * dims} if dims else {}
    return pltpu.CompilerParams(vmem_limit_bytes=limit_mib * 1024 * 1024, **semantics)


def groups(sizes):
    nz, ny, nx = sizes

    def place(z, y, x):
        return (z * ny + y) * nx + x

    pair = 2
    near = [[place(q * pair + h, y, x) for h in range(pair) for y in range(ny) for x in range(nx)] for q in range(nz // pair)]
    far = [[place(q * pair + h, y, x) for q in range(nz // pair)] for h in range(pair) for y in range(ny) for x in range(nx)]
    return near, far


VMEM = pl.BlockSpec(memory_space=pltpu.VMEM)
HBM = pl.BlockSpec(memory_space=pltpu.HBM)


def make_body(near, far):
    def body(spectra, inverse_var, mask_bits, sky_flags, fiber_ids, positions, throughput):
        exposures, fibers, waves = spectra.shape
        f32 = jnp.float32
        stacked = -(-12 * fibers // LANES) * LANES
        moved = 4 * exposures * fibers * waves

        held = [
            pltpu.with_memory_space_constraint(value, pltpu.HBM)
            for value in (fiber_ids, positions, throughput, sky_flags, spectra, inverse_var, mask_bits)
        ]
        packed, feats, flux, weight = pl.pallas_call(
            moments_kernel,
            in_specs=[HBM] * 7,
            out_specs=[VMEM] * 4,
            out_shape=[
                jax.ShapeDtypeStruct((waves // LANES * PACKED, LANES), f32),
                jax.ShapeDtypeStruct((2 * fibers, LANES), f32),
                jax.ShapeDtypeStruct(spectra.shape, f32),
                jax.ShapeDtypeStruct(spectra.shape, f32),
            ],
            scratch_shapes=[
                pltpu.VMEM(fiber_ids.shape, jnp.int32),
                pltpu.VMEM(positions.shape, f32),
                pltpu.VMEM((exposures, fibers), f32),
                pltpu.VMEM((exposures, fibers), jnp.int32),
                pltpu.VMEM(spectra.shape, f32),
                pltpu.VMEM(spectra.shape, jnp.int32),
                pltpu.VMEM((80, stacked), jnp.bfloat16),
                pltpu.VMEM((stacked, LANES), f32),
                pltpu.SemaphoreType.DMA((4,)),
                pltpu.SemaphoreType.DMA((len(GRAINS), 3)),
            ],
            compiler_params=params(20),
            cost_estimate=cost(FLOPS, 3 * moved),
            name="moments",
        )(*held)

        members = len(near[0])
        packed = packed.reshape(members, PACKED, 1, LANES)
        arrived = lax.all_to_all(packed, "fiber", 0, 0, axis_index_groups=near, tiled=True)
        copies = pl.pallas_call(
            add_kernel,
            out_shape=jax.ShapeDtypeStruct((len(far[0]), ROWS, LANES), f32),
            compiler_params=params(8),
            name="add",
        )(arrived.reshape(members * PACKED, LANES))
        parts = lax.all_to_all(copies, "fiber", 0, 0, axis_index_groups=far, tiled=True)
        solved = pl.pallas_call(
            solve_kernel,
            out_shape=jax.ShapeDtypeStruct((members, PARAMS, LANES), f32),
            compiler_params=params(8),
            name="solve",
        )(parts, jnp.asarray(rebuild_rows(), f32))
        coeffs = lax.all_to_all(solved, "fiber", 0, 0, axis_index_groups=near, tiled=True)

        chi_local, late, residual, sky_coeffs = pl.pallas_call(
            residual_kernel,
            in_specs=[VMEM] * 4,
            out_specs=[VMEM, VMEM, HBM, HBM],
            out_shape=[
                jax.ShapeDtypeStruct((8, exposures * fibers), f32),
                jax.ShapeDtypeStruct((exposures, fibers, waves - EARLY), f32),
                jax.ShapeDtypeStruct(spectra.shape, f32),
                jax.ShapeDtypeStruct((PARAMS, waves), f32),
            ],
            scratch_shapes=[
                pltpu.VMEM((exposures * fibers, LANES), f32),
                pltpu.VMEM((exposures, fibers, EARLY), f32),
                pltpu.VMEM((PARAMS, waves), f32),
                pltpu.SemaphoreType.DMA((EARLY // WRITE,)),
                pltpu.SemaphoreType.DMA,
            ],
            compiler_params=params(16),
            cost_estimate=cost(FLOPS, moved),
            name="residual",
        )(feats, coeffs, flux, weight)
        halves = lax.axis_size("wave")
        chi_other = lax.ppermute(chi_local, "wave", [(h, (h + 1) % halves) for h in range(halves)])
        residual = pl.pallas_call(
            late_kernel,
            in_specs=[VMEM, HBM],
            out_specs=HBM,
            out_shape=jax.ShapeDtypeStruct(spectra.shape, f32),
            input_output_aliases={1: 0},
            scratch_shapes=[pltpu.SemaphoreType.DMA((exposures,))],
            compiler_params=params(4),
            cost_estimate=cost(FLOPS, moved),
            name="late",
        )(late, residual)
        chi_square = pl.pallas_call(
            functools.partial(chi_kernel, 1.0 / (waves * halves)),
            out_shape=jax.ShapeDtypeStruct((exposures, fibers), f32),
            compiler_params=params(4),
            name="chi",
        )(chi_local, chi_other)
        return residual, chi_square, sky_coeffs

    return body


def solution(mesh):
    near, far = groups((8, 4, 4))
    placed = (
        P(None, "fiber", "wave"),
        P(None, "fiber", "wave"),
        P(None, "fiber", "wave"),
        P(None, "fiber"),
        P("fiber"),
        P(),
        P(None, "fiber"),
    )
    return jax.shard_map(
        make_body(near, far),
        mesh=mesh,
        in_specs=placed,
        out_specs=(P(None, "fiber", "wave"), P(None, "fiber"), P(None, "wave")),
        check_vma=False,
    )
```

```python
import functools

import jax
import jax.numpy as jnp
from jax import lax
from jax.experimental import pallas as pl
from jax.experimental.pallas import tpu as pltpu
from jax.sharding import PartitionSpec as P

PARAMS = 16
BAD_BITS = 31
PRIOR = 1.0
MOMENTS = 7
BASIS = 4
RIGHT_ROW = 49
PACKED = 65
ROWS = 72
LANES = 128
PIECE = 512
WRITE = 1024
EARLY = 1024
MIDDLE = 1536
GRAINS = (2048, 2048)
FLOPS = 4_000_000_000


def legendre_series(coord, total):
    series = [jnp.ones_like(coord), coord]
    for order in range(1, total - 1):
        series.append(((2 * order + 1) * coord * series[order] - order * series[order - 1]) / (order + 1))
    return series


def monomial_table(total):
    coeffs = [[0.0] * total for _ in range(total)]
    coeffs[0][0] = 1.0
    coeffs[1][1] = 1.0
    for order in range(1, total - 1):
        for power in range(total):
            raised = coeffs[order][power - 1] if power >= 1 else 0.0
            coeffs[order + 1][power] = ((2 * order + 1) * raised - order * coeffs[order - 1][power]) / (order + 1)
    return coeffs


def product_series(higher, first, second):
    product = [0.0] * MOMENTS
    for left in range(MOMENTS):
        for right in range(MOMENTS - left):
            product[left + right] += higher[first][left] * higher[second][right]
    series = [0.0] * MOMENTS
    for order in reversed(range(MOMENTS)):
        now = product[order] / higher[order][order]
        series[order] = now
        for power in range(MOMENTS):
            product[power] -= now * higher[order][power]
    return series


def rebuild_rows():
    higher = monomial_table(MOMENTS)
    pair = [[product_series(higher, a, b) for b in range(BASIS)] for a in range(BASIS)]
    rows = []
    for i in range(BASIS):
        for j in range(BASIS):
            for k in range(BASIS):
                for l in range(BASIS):
                    row = [0.0] * LANES
                    for a in range(MOMENTS):
                        for b in range(MOMENTS):
                            row[a * MOMENTS + b] = pair[i][k][a] * pair[j][l][b]
                    rows.append(row)
    return rows


def split3(value):
    high = value.astype(jnp.bfloat16)
    rest = value - high.astype(jnp.float32)
    middle = rest.astype(jnp.bfloat16)
    low = (rest - middle.astype(jnp.float32)).astype(jnp.bfloat16)
    return high, middle, low


def dot6(left, right):
    l1, l2, l3 = split3(left)
    r1, r2, r3 = split3(right)
    total = None
    for a, b in ((l1, r3), (l3, r1), (l2, r2), (l1, r2), (l2, r1), (l1, r1)):
        part = jnp.dot(a, b, preferred_element_type=jnp.float32)
        total = part if total is None else total + part
    return total


def build_features(ids_ref, pos_ref, tput_ref, sky_ref, stack_ref, feat_ref, left_ref):
    exposures, fibers = tput_ref.shape
    stack_ref[0:LANES, :] = jnp.zeros((LANES, LANES), jnp.float32)
    stack_ref[0:exposures, 0:fibers] = tput_ref[...]
    stack_ref[8:8 + exposures, 0:fibers] = sky_ref[...].astype(jnp.float32)
    stack_ref[16:17, 0:fibers] = ids_ref[...].reshape(1, fibers).astype(jnp.float32)
    turned = stack_ref[0:LANES, :].T
    lane = lax.broadcasted_iota(jnp.int32, (fibers, LANES), 1)
    ids = jnp.broadcast_to(turned[0:fibers, 16:17], (fibers, LANES)).astype(jnp.int32)
    sum_x = jnp.zeros((fibers, LANES), jnp.float32)
    sum_y = jnp.zeros((fibers, LANES), jnp.float32)
    offset = ids - lane
    for tile in range(pos_ref.shape[1] // LANES):
        hit = offset == tile * LANES
        cut = slice(tile * LANES, (tile + 1) * LANES)
        sum_x = jnp.where(hit, pos_ref[0:1, cut], sum_x)
        sum_y = jnp.where(hit, pos_ref[1:2, cut], sum_y)
    coord_x = jnp.sum(sum_x, axis=1, keepdims=True)
    coord_y = jnp.sum(sum_y, axis=1, keepdims=True)
    series_x = legendre_series(jnp.broadcast_to(coord_x, (fibers, LANES)), MOMENTS)
    series_y = legendre_series(jnp.broadcast_to(coord_y, (fibers, LANES)), MOMENTS)
    is_right = lane >= RIGHT_ROW

    def products(index_x, index_y):
        along_x = jnp.zeros((fibers, LANES), jnp.float32)
        along_y = jnp.zeros((fibers, LANES), jnp.float32)
        for order in range(MOMENTS):
            along_x = jnp.where(index_x == order, series_x[order], along_x)
            along_y = jnp.where(index_y == order, series_y[order], along_y)
        return along_x * along_y

    product = products(
        jnp.where(is_right, (lane - RIGHT_ROW) // BASIS, lane // MOMENTS),
        jnp.where(is_right, (lane - RIGHT_ROW) % BASIS, lane % MOMENTS),
    )
    group = lane // PARAMS
    model_parts = [part.astype(jnp.float32) for part in split3(products(lane % PARAMS // BASIS, lane % BASIS))]
    model_left = jnp.where((group == 1) | (group == 4), model_parts[1], jnp.where(group == 2, model_parts[2], model_parts[0]))
    moment_part = jnp.where(lane < MOMENTS * MOMENTS, product, 0.0)
    right_part = jnp.where(is_right & (lane < RIGHT_ROW + PARAMS), product, 0.0)
    feat_ref[0:fibers, :] = model_left
    feat_ref[fibers:2 * fibers, :] = turned[0:fibers, :]
    both = jnp.concatenate([moment_part, right_part], axis=0)
    high, middle, low = (part.astype(jnp.float32) for part in split3(both))
    rows = 2 * fibers
    for place, part in enumerate((high, middle, low, high, middle, high)):
        stack_ref[place * rows:(place + 1) * rows, :] = part
    stack_ref[6 * rows:, :] = jnp.zeros((stack_ref.shape[0] - 6 * rows, LANES), jnp.float32)
    for tile in range(stack_ref.shape[0] // LANES):
        cut = slice(tile * LANES, (tile + 1) * LANES)
        left_ref[:, cut] = stack_ref[cut, :].T[0:left_ref.shape[0], :].astype(jnp.bfloat16)


def piece_copies(flux_hbm, ivar_hbm, bits_hbm, flux_ref, ivar_ref, bits_ref, sems):
    copies = {}
    begin = 0
    for place, width in enumerate(GRAINS):
        cut = pl.ds(begin, width)
        copies[begin] = [
            pltpu.make_async_copy(source.at[:, :, cut], target.at[:, :, cut], sems.at[place, which])
            for which, (source, target) in enumerate(((flux_hbm, flux_ref), (ivar_hbm, ivar_ref), (bits_hbm, bits_ref)))
        ]
        begin += width
    return copies


def sum_pieces(copies, feat_ref, left_ref, flux_ref, ivar_ref, bits_ref, out_ref, weight_ref):
    exposures, fibers, _ = flux_ref.shape
    columns = feat_ref[fibers:2 * fibers, :]
    for piece in range(flux_ref.shape[2] // PIECE):
        for copy in copies.get(piece * PIECE, ()):
            copy.wait()
        here = slice(piece * PIECE, (piece + 1) * PIECE)
        moment_rows = None
        right_rows = None
        for e in range(exposures):
            through = columns[:, e:e + 1]
            sky = columns[:, 8 + e:9 + e]
            weight = jnp.where((bits_ref[e, :, here] & BAD_BITS) == 0, ivar_ref[e, :, here], 0.0)
            weight_ref[e, :, here] = weight
            first = weight * (through * sky)
            a = first * through
            b = first * flux_ref[e, :, here]
            moment_rows = a if e == 0 else moment_rows + a
            right_rows = b if e == 0 else right_rows + b
        high, middle, low = split3(jnp.concatenate([moment_rows, right_rows], axis=0))
        right = jnp.concatenate([high, high, high, middle, middle, low], axis=0)
        sums = jnp.dot(left_ref[:, 0:right.shape[0]], right, preferred_element_type=jnp.float32)
        for k in range(PIECE // LANES):
            chunk = piece * (PIECE // LANES) + k
            out_ref[chunk * PACKED:(chunk + 1) * PACKED, :] = sums[0:PACKED, k * LANES:(k + 1) * LANES]


def moments_kernel(ids_hbm, pos_hbm, tput_hbm, sky_hbm, flux_hbm, ivar_hbm, bits_hbm, out_ref, feat_ref, flux_ref, weight_ref,
                   ids_ref, pos_ref, tput_ref, sky_ref, ivar_ref, bits_ref, left_ref, stack_ref, small_sems, sems):
    small = [
        pltpu.make_async_copy(source, target, small_sems.at[place])
        for place, (source, target) in enumerate(((ids_hbm, ids_ref), (pos_hbm, pos_ref), (tput_hbm, tput_ref), (sky_hbm, sky_ref)))
    ]
    for copy in small:
        copy.start()
    copies = piece_copies(flux_hbm, ivar_hbm, bits_hbm, flux_ref, ivar_ref, bits_ref, sems)
    for begin, trio in copies.items():
        for which, copy in enumerate(trio):
            copy.start(priority=(which + (begin > 0)) % 2)
    for copy in small:
        copy.wait()
    build_features(ids_ref, pos_ref, tput_ref, sky_ref, stack_ref, feat_ref, left_ref)
    sum_pieces(copies, feat_ref, left_ref, flux_ref, ivar_ref, bits_ref, out_ref, weight_ref)


def add_kernel(in_ref, out_ref):
    total = in_ref[0:PACKED, :]
    for source in range(1, in_ref.shape[0] // PACKED):
        total = total + in_ref[source * PACKED:(source + 1) * PACKED, :]
    total = jnp.concatenate([total, jnp.zeros((ROWS - PACKED, LANES), jnp.float32)], axis=0)
    for target in range(out_ref.shape[0]):
        out_ref[target] = total


def solve_kernel(in_ref, table_ref, out_ref):
    total = in_ref[0]
    for source in range(1, in_ref.shape[0]):
        total = total + in_ref[source]
    normal = dot6(table_ref[...], jnp.concatenate([total, jnp.zeros((LANES - ROWS, LANES), jnp.float32)], axis=0))
    sub = lax.broadcasted_iota(jnp.int32, (PARAMS, LANES), 0)
    columns = []
    for k in range(PARAMS):
        column = normal[k * PARAMS:(k + 1) * PARAMS]
        columns.append(jnp.where(sub == k, column + PRIOR, column))
    right = total[RIGHT_ROW:RIGHT_ROW + PARAMS]
    scale = jnp.zeros((PARAMS, LANES), jnp.float32)
    for j in range(PARAMS):
        inverse = 1.0 / columns[j][j:j + 1]
        scale = jnp.where(sub == j, inverse, scale)
        factor = jnp.where(sub == j, 0.0, columns[j] * inverse)
        for l in range(j + 1, PARAMS):
            columns[l] = columns[l] - factor * columns[l][j:j + 1]
        right = right - factor * right[j:j + 1]
    solved = right * scale
    for target in range(out_ref.shape[0]):
        out_ref[target] = solved


def joined(coeff_ref, first, count):
    return jnp.concatenate([coeff_ref[first + k] for k in range(count)], axis=1)


def residual_kernel(feat_ref, coeff_ref, flux_ref, weight_ref, chi_ref, late_ref, res_hbm, all_hbm, sum_ref, early_ref, all_ref, sems, all_sem):
    exposures, fibers, waves = flux_ref.shape
    chunks = waves // LANES
    early = early_ref.shape[2]
    all_ref[...] = joined(coeff_ref, 0, chunks)
    copies = [pltpu.make_async_copy(all_ref, all_hbm, all_sem)]
    copies[0].start(priority=1)
    basis = feat_ref[0:fibers, 0:6 * PARAMS].astype(jnp.bfloat16)
    sums = [None] * exposures
    for piece in range(waves // PIECE):
        here = slice(piece * PIECE, (piece + 1) * PIECE)
        high, middle, low = split3(joined(coeff_ref, piece * (PIECE // LANES), PIECE // LANES))
        model = jnp.dot(basis, jnp.concatenate([high, high, high, middle, middle, low], axis=0), preferred_element_type=jnp.float32)
        for e in range(exposures):
            residual = flux_ref[e, :, here] - feat_ref[fibers:2 * fibers, e:e + 1] * model
            if piece * PIECE < early:
                early_ref[e, :, here] = residual
            else:
                late_ref[e, :, piece * PIECE - early:(piece + 1) * PIECE - early] = residual
            chi = weight_ref[e, :, here] * residual * residual
            for k in range(PIECE // LANES):
                part = chi[:, k * LANES:(k + 1) * LANES]
                sums[e] = part if sums[e] is None else sums[e] + part
        done = (piece + 1) * PIECE
        if done <= early and done % WRITE == 0:
            cut = pl.ds(done - WRITE, WRITE)
            copies.append(pltpu.make_async_copy(early_ref.at[:, :, cut], res_hbm.at[:, :, cut], sems.at[done // WRITE - 1]))
            copies[-1].start(priority=done // WRITE % 2)
    for e in range(exposures):
        sum_ref[e * fibers:(e + 1) * fibers, :] = sums[e]
    ones = jnp.ones((8, LANES), jnp.float32)
    chi_ref[...] = lax.dot_general(ones, sum_ref[...], (((1,), (1,)), ((), ())), precision=lax.Precision.HIGHEST, preferred_element_type=jnp.float32)
    for copy in copies:
        copy.wait()


def late_copies(late_ref, res_hbm, first, width, sems):
    begin = res_hbm.shape[2] - late_ref.shape[2] + first
    return [
        pltpu.make_async_copy(late_ref.at[e, :, pl.ds(first, width)], res_hbm.at[e, :, pl.ds(begin, width)], sems.at[e])
        for e in range(late_ref.shape[0])
    ]


def middle_kernel(late_ref, _, res_hbm, sems):
    copies = late_copies(late_ref, res_hbm, 0, MIDDLE, sems)
    for e, copy in enumerate(copies):
        copy.start(priority=e % 2)
    for copy in copies:
        copy.wait()


def finish_kernel(scale, late_ref, mine_ref, other_ref, _, res_hbm, out_hbm, out_ref, sems, out_sem):
    copies = late_copies(late_ref, res_hbm, MIDDLE, late_ref.shape[2] - MIDDLE, sems)
    for e, copy in enumerate(copies):
        copy.start(priority=e % 2)
    exposures, fibers = out_ref.shape
    total = (mine_ref[...] + other_ref[...]) * scale
    for e in range(exposures):
        out_ref[e:e + 1, :] = total[0:1, e * fibers:(e + 1) * fibers]
    copies.append(pltpu.make_async_copy(out_ref, out_hbm, out_sem))
    copies[-1].start(priority=1)
    for copy in copies:
        copy.wait()


def cost(flops, moved):
    return pl.CostEstimate(flops=flops, bytes_accessed=moved, transcendentals=0)


def params(limit_mib, dims=0):
    semantics = {"dimension_semantics": ("arbitrary",) * dims} if dims else {}
    return pltpu.CompilerParams(vmem_limit_bytes=limit_mib * 1024 * 1024, **semantics)


def groups(sizes):
    nz, ny, nx = sizes

    def place(z, y, x):
        return (z * ny + y) * nx + x

    pair = 2
    near = [[place(q * pair + h, y, x) for h in range(pair) for y in range(ny) for x in range(nx)] for q in range(nz // pair)]
    far = [[place(q * pair + h, y, x) for q in range(nz // pair)] for h in range(pair) for y in range(ny) for x in range(nx)]
    return near, far


VMEM = pl.BlockSpec(memory_space=pltpu.VMEM)
HBM = pl.BlockSpec(memory_space=pltpu.HBM)


def make_body(near, far):
    def body(spectra, inverse_var, mask_bits, sky_flags, fiber_ids, positions, throughput):
        exposures, fibers, waves = spectra.shape
        f32 = jnp.float32
        stacked = -(-12 * fibers // LANES) * LANES
        moved = 4 * exposures * fibers * waves

        held = [
            pltpu.with_memory_space_constraint(value, pltpu.HBM)
            for value in (fiber_ids, positions, throughput, sky_flags, spectra, inverse_var, mask_bits)
        ]
        packed, feats, flux, weight = pl.pallas_call(
            moments_kernel,
            in_specs=[HBM] * 7,
            out_specs=[VMEM] * 4,
            out_shape=[
                jax.ShapeDtypeStruct((waves // LANES * PACKED, LANES), f32),
                jax.ShapeDtypeStruct((2 * fibers, LANES), f32),
                jax.ShapeDtypeStruct(spectra.shape, f32),
                jax.ShapeDtypeStruct(spectra.shape, f32),
            ],
            scratch_shapes=[
                pltpu.VMEM(fiber_ids.shape, jnp.int32),
                pltpu.VMEM(positions.shape, f32),
                pltpu.VMEM((exposures, fibers), f32),
                pltpu.VMEM((exposures, fibers), jnp.int32),
                pltpu.VMEM(spectra.shape, f32),
                pltpu.VMEM(spectra.shape, jnp.int32),
                pltpu.VMEM((80, stacked), jnp.bfloat16),
                pltpu.VMEM((stacked, LANES), f32),
                pltpu.SemaphoreType.DMA((4,)),
                pltpu.SemaphoreType.DMA((len(GRAINS), 3)),
            ],
            compiler_params=params(20),
            cost_estimate=cost(FLOPS, 3 * moved),
            name="moments",
        )(*held)

        members = len(near[0])
        packed = packed.reshape(members, PACKED, 1, LANES)
        arrived = lax.all_to_all(packed, "fiber", 0, 0, axis_index_groups=near, tiled=True)
        copies = pl.pallas_call(
            add_kernel,
            out_shape=jax.ShapeDtypeStruct((len(far[0]), ROWS, LANES), f32),
            compiler_params=params(8),
            name="add",
        )(arrived.reshape(members * PACKED, LANES))
        parts = lax.all_to_all(copies, "fiber", 0, 0, axis_index_groups=far, tiled=True)
        solved = pl.pallas_call(
            solve_kernel,
            out_shape=jax.ShapeDtypeStruct((members, PARAMS, LANES), f32),
            compiler_params=params(8),
            name="solve",
        )(parts, jnp.asarray(rebuild_rows(), f32))
        coeffs = lax.all_to_all(solved, "fiber", 0, 0, axis_index_groups=near, tiled=True)

        chi_local, late, residual, sky_coeffs = pl.pallas_call(
            residual_kernel,
            in_specs=[VMEM] * 4,
            out_specs=[VMEM, VMEM, HBM, HBM],
            out_shape=[
                jax.ShapeDtypeStruct((8, exposures * fibers), f32),
                jax.ShapeDtypeStruct((exposures, fibers, waves - EARLY), f32),
                jax.ShapeDtypeStruct(spectra.shape, f32),
                jax.ShapeDtypeStruct((PARAMS, waves), f32),
            ],
            scratch_shapes=[
                pltpu.VMEM((exposures * fibers, LANES), f32),
                pltpu.VMEM((exposures, fibers, EARLY), f32),
                pltpu.VMEM((PARAMS, waves), f32),
                pltpu.SemaphoreType.DMA((EARLY // WRITE,)),
                pltpu.SemaphoreType.DMA,
            ],
            compiler_params=params(16),
            cost_estimate=cost(FLOPS, moved),
            name="residual",
        )(feats, coeffs, flux, weight)
        halves = lax.axis_size("wave")
        chi_other = lax.ppermute(chi_local, "wave", [(h, (h + 1) % halves) for h in range(halves)])
        residual = pl.pallas_call(
            middle_kernel,
            in_specs=[VMEM, HBM],
            out_specs=HBM,
            out_shape=jax.ShapeDtypeStruct(spectra.shape, f32),
            input_output_aliases={1: 0},
            scratch_shapes=[pltpu.SemaphoreType.DMA((exposures,))],
            compiler_params=params(4),
            cost_estimate=cost(FLOPS, moved),
            name="middle",
        )(late, residual)
        residual, chi_square = pl.pallas_call(
            functools.partial(finish_kernel, 1.0 / (waves * halves)),
            in_specs=[VMEM, VMEM, VMEM, HBM],
            out_specs=[HBM, HBM],
            out_shape=[
                jax.ShapeDtypeStruct(spectra.shape, f32),
                jax.ShapeDtypeStruct((exposures, fibers), f32),
            ],
            input_output_aliases={3: 0},
            scratch_shapes=[
                pltpu.VMEM((exposures, fibers), f32),
                pltpu.SemaphoreType.DMA((exposures,)),
                pltpu.SemaphoreType.DMA,
            ],
            compiler_params=params(4),
            name="finish",
        )(late, chi_local, chi_other, residual)
        return residual, chi_square, sky_coeffs

    return body


def solution(mesh):
    near, far = groups((8, 4, 4))
    placed = (
        P(None, "fiber", "wave"),
        P(None, "fiber", "wave"),
        P(None, "fiber", "wave"),
        P(None, "fiber"),
        P("fiber"),
        P(),
        P(None, "fiber"),
    )
    return jax.shard_map(
        make_body(near, far),
        mesh=mesh,
        in_specs=placed,
        out_specs=(P(None, "fiber", "wave"), P(None, "fiber"), P(None, "wave")),
        check_vma=False,
    )
```
